256 devices in a mesh: row: 16 (over y_lo, x, core), col: 16 (over y_hi, z).
Axes of the slice: x: 4, y: 4 (y_hi: 2, y_lo: 2; y = y_hi * 2 + y_lo), z: 8, core: 2. Of those that a mesh axis runs over, the one named last changes fastest.
Arguments:
- objects: float32 [4, 8192, 8192], P(None, 'row', 'col'), may hold values from -1 to 1, as said below
- probe: float32 [2, 256, 256], replicated, may hold values from -6 to 6
- kernel: float32 [2, 256, 256], replicated, may hold values from -1 to 1, as said below
- measured: float32 [16, 16, 9, 256, 256], P('row', 'col'), may hold values from 0.3 to 3
- offsets: int32 [16, 16, 9, 2], P('row', 'col'), may hold values from -64 to 320, as said below
Outputs:
- updated: float32 [4, 8192, 8192], P(None, 'row', 'col')
The draws below stay inside these ranges and needn't reach their ends.
Inputs may be any that keep to these rules, and one draw needn't show every extreme that they name: Every window lies inside the object: tiles in the first row or column have offsets of 0 or more there, tiles in the last have offsets of at most 256 there. `objects`: real and imaginary parts of each slice give a magnitude between 0.6 and 1. `kernel`: each entry has magnitude 1.
All inputs are finite; a program needn't handle non-finite values.
Results may differ from the reference program's by a relative error of at most 0.012.
Values sent between devices are 32-bit elements; how exact they have to be, the bound alone decides.
A program may use at most 128 MiB of HBM per device.

```python
import math
import jax
import jax.numpy as jnp
from jax import lax

W = 256
TILE = 512
HALO = 64
POS = 9
TILES_R = 16
TILES_C = 16
IMG_Y = 8192
IMG_X = 8192


def draw_objects(key, part):
    key_amp = jax.random.fold_in(key, 101)
    key_phase = jax.random.fold_in(key, 202)
    amplitude = jax.random.uniform(key_amp, (2, IMG_Y, IMG_X), jnp.float32, 0.6, 1.0)
    phase = jax.random.uniform(key_phase, (2, IMG_Y, IMG_X), jnp.float32, -1.5, 1.5)
    return jnp.stack([amplitude[0] * jnp.cos(phase[0]), amplitude[0] * jnp.sin(phase[0]), amplitude[1] * jnp.cos(phase[1]), amplitude[1] * jnp.sin(phase[1])])


def draw_kernel(key, part):
    phase = jax.random.uniform(jax.random.fold_in(key, 303), (W, W), jnp.float32, -3.14159, 3.14159)
    return jnp.stack([jnp.cos(phase), jnp.sin(phase)])


def lattice_offset(level, low, high, jitter, span):
    middle = (TILE - W) // 2 + jitter - span // 2
    first = low + jitter
    last = high - jitter
    return jnp.where(level == 0, first, jnp.where(level == 1, middle, last))


def draw_offsets(key, part):
    rows = jnp.arange(TILES_R, dtype=jnp.int32)[:, None, None]
    cols = jnp.arange(TILES_C, dtype=jnp.int32)[None, :, None]
    which = jnp.arange(POS, dtype=jnp.int32)[None, None, :]
    low_r = jnp.where(rows == 0, 0, -HALO)
    high_r = jnp.where(rows == TILES_R - 1, TILE - W, TILE - W + HALO)
    low_c = jnp.where(cols == 0, 0, -HALO)
    high_c = jnp.where(cols == TILES_C - 1, TILE - W, TILE - W + HALO)
    span = HALO // 2
    jitter_y = jax.random.randint(jax.random.fold_in(key, 404), (TILES_R, TILES_C, POS), 0, span)
    jitter_x = jax.random.randint(jax.random.fold_in(key, 505), (TILES_R, TILES_C, POS), 0, span)
    level_y = which // 3
    level_x = which % 3
    offset_y = lattice_offset(level_y, low_r, high_r, jitter_y, span)
    offset_x = lattice_offset(level_x, low_c, high_c, jitter_x, span)
    return jnp.stack([offset_y, offset_x], -1).astype(jnp.int32)


def block_levels(stream_key, shape, shards, least, largest):
    level, own = 1.0, jax.random.fold_in(stream_key, 6)
    for dim, shards_of in shards:
        heights = jnp.exp(jax.random.uniform(jax.random.fold_in(own, dim), (shards_of,), jnp.float32, least / len(shards), largest / len(shards)))
        level = level * jnp.repeat(heights, shape[dim] // shards_of).reshape([-1 if axis == dim else 1 for axis in range(len(shape))])
    return level


def bell_draw(stream_key, extent, scale, limit, held_as=jnp.bfloat16):
    array = jax.random.normal(stream_key, extent, jnp.float32) * scale
    return jnp.minimum(jnp.maximum(array, -limit), limit).astype(held_as)


def setup_inputs(seed: int = 0) -> dict:
    streams_of = jax.random.split(jax.random.key(seed), 6)
    return {
        "objects": draw_objects(jax.random.fold_in(streams_of[5], 71), 0),
        "probe": bell_draw(streams_of[1], (2, W, W), 1.0, 6.0, jnp.float32),
        "kernel": draw_kernel(jax.random.fold_in(streams_of[5], 71), 0),
        "measured": jnp.clip(jnp.exp(math.log(3.0) - 2.3025851 * jax.random.uniform(streams_of[3], (TILES_R, TILES_C, POS, W, W), jnp.float32) ** block_levels(streams_of[3], (TILES_R, TILES_C, POS, W, W), ((0, 16), (1, 16)), -0.2, 0.2)), 0.3, 3.0),
        "offsets": draw_offsets(jax.random.fold_in(streams_of[5], 71), 0),
    }


RATE = 0.5

def make_tables(width):
    index = jnp.arange(width, dtype=jnp.int32)
    product = index[:, None] * index[None, :] % width
    angle = 2.0 * jnp.pi / width * product.astype(jnp.float32)
    norm = 1.0 / jnp.sqrt(jnp.float32(width))
    cosine = jnp.cos(angle) * norm
    sine = jnp.sin(angle) * norm

    def blocks(real_part, imag_part):
        left = jnp.concatenate([jnp.concatenate([real_part, -imag_part], 1), jnp.concatenate([imag_part, real_part], 1)], 0)
        right = jnp.concatenate([jnp.concatenate([real_part, imag_part], 1), jnp.concatenate([-imag_part, real_part], 1)], 0)
        return (left.astype(jnp.bfloat16), right.astype(jnp.bfloat16))
    return (blocks(cosine, -sine), blocks(cosine, sine))

def transform(real_part, imag_part, table):
    left, right = table
    width = real_part.shape[0]
    stacked = jnp.concatenate([real_part, imag_part], 0).astype(jnp.bfloat16)
    first = jnp.dot(left, stacked, preferred_element_type=jnp.float32)
    middle = jnp.concatenate([first[:width], first[width:]], 1).astype(jnp.bfloat16)
    result = jnp.dot(middle, right, preferred_element_type=jnp.float32)
    return (result[:, :width], result[:, width:])

def position_gradient(window, probe, kernel, amplitude, tables):
    forward, inverse = tables
    o1r, o1i, o2r, o2i = (window[0], window[1], window[2], window[3])
    pr, pim = (probe[0], probe[1])
    kr, kim = (kernel[0], kernel[1])
    ar = pr * o1r - pim * o1i
    ai = pr * o1i + pim * o1r
    fr, fi = transform(ar, ai, forward)
    br = kr * fr - kim * fi
    bi = kr * fi + kim * fr
    sr, si = transform(br, bi, inverse)
    er = sr * o2r - si * o2i
    ei = sr * o2i + si * o2r
    zr, zi = transform(er, ei, forward)
    factor = 1.0 - amplitude / jnp.sqrt(zr * zr + zi * zi + 1.0)
    gr, gi = transform(zr * factor, zi * factor, inverse)
    g2r = sr * gr + si * gi
    g2i = sr * gi - si * gr
    hr = o2r * gr + o2i * gi
    hi = o2r * gi - o2i * gr
    ur, ui = transform(hr, hi, forward)
    vr = kr * ur + kim * ui
    vi = kr * ui - kim * ur
    wr, wi = transform(vr, vi, inverse)
    g1r = pr * wr + pim * wi
    g1i = pr * wi - pim * wr
    return jnp.stack([g1r, g1i, g2r, g2i])

def reference(objects, probe, kernel, measured, offsets):
    tables = make_tables(W)
    count = TILES_R * TILES_C * POS
    items = jnp.arange(count, dtype=jnp.int32)
    tile_row = items // (TILES_C * POS)
    tile_col = items // POS % TILES_C
    flat_offsets = offsets.reshape(count, 2)
    anchor_y = (tile_row * TILE + flat_offsets[:, 0]).astype(jnp.int32)
    anchor_x = (tile_col * TILE + flat_offsets[:, 1]).astype(jnp.int32)
    amplitudes = measured.reshape(count, W, W)
    zero = jnp.zeros((), jnp.int32)

    def step(gradient, item):
        top, left, amplitude = item
        window = lax.dynamic_slice(objects, (zero, top, left), (4, W, W))
        piece = position_gradient(window, probe, kernel, amplitude, tables)
        current = lax.dynamic_slice(gradient, (zero, top, left), (4, W, W))
        gradient = lax.dynamic_update_slice(gradient, current + piece, (zero, top, left))
        return (gradient, None)
    gradient, _ = lax.scan(step, jnp.zeros_like(objects), (anchor_y, anchor_x, amplitudes))
    return objects - RATE * gradient
```

```python
import functools

import jax
import jax.numpy as jnp
import numpy as np
from jax import lax
from jax.experimental import pallas as pl
from jax.experimental.pallas import tpu as pltpu
from jax.sharding import PartitionSpec as P

HALO = 64
RATE = 0.5
LANES = 128
HALF = 64
MESH = pl.DeviceIdType.MESH
BF16 = jnp.bfloat16
F32 = jnp.float32
ANY = pl.BlockSpec(memory_space=pl.ANY)


@functools.cache
def tables(width):
    index = np.arange(width)
    angle = 2.0 * np.pi / width * (index[:, None] * index[None, :] % width)
    norm = 1.0 / np.sqrt(width)
    cosine = (np.cos(angle) * norm).astype(np.float32)
    sine = (np.sin(angle) * norm).astype(np.float32)

    def left(r, i):
        return np.concatenate(
            [np.concatenate([r, -i], 1), np.concatenate([i, r], 1)], 0
        ).astype(BF16)

    def right(r, i):
        return np.concatenate(
            [np.concatenate([r, i], 1), np.concatenate([-i, r], 1)], 0
        ).astype(BF16)

    h = width // 2
    split = []
    for parity in (0, 1):
        split.append(left(cosine[parity::2, :h], -sine[parity::2, :h]))
    for parity in (0, 1):
        split.append(left(cosine[:h, parity::2], sine[:h, parity::2]))
    return np.stack(split), np.stack([right(cosine, -sine), right(cosine, sine)])


def lane_index(shape):
    return lax.broadcasted_iota(jnp.int32, shape, len(shape) - 1)


def pack_high(re, im):
    return jnp.where(lane_index(re.shape) < HALF, pltpu.roll(re, HALF, re.ndim - 1), im)


def pack_low(re, im):
    return jnp.where(lane_index(re.shape) < HALF, re, pltpu.roll(im, HALF, im.ndim - 1))


def pack_kernel(left_ref, right_ref, low_ref, high_ref):
    for s in range(2):
        low_ref[s] = pack_low(left_ref[2 * s], left_ref[2 * s + 1])
        high_ref[s] = pack_high(right_ref[2 * s], right_ref[2 * s + 1])


def pack_edges(objects):
    tile = objects.shape[1]
    last = objects.shape[2] // LANES - 1
    return pl.pallas_call(
        pack_kernel,
        grid=(1,),
        out_shape=[jax.ShapeDtypeStruct((2, tile, LANES), F32)] * 2,
        in_specs=[
            pl.BlockSpec((4, tile, LANES), lambda i: (0, 0, 0)),
            pl.BlockSpec((4, tile, LANES), lambda i: (0, 0, last)),
        ],
        out_specs=[pl.BlockSpec((2, tile, LANES), lambda i: (0, 0, 0))] * 2,
    )(objects, objects)


def exchange_kernel(base, first, rows, cols, up_src, down_src, left_src, right_src,
                    from_up, from_down, from_left, from_right, send, recv):
    tile = rows
    me_r, me_c = lax.axis_index("row"), lax.axis_index("col")
    n_r, n_c = lax.axis_size("row"), lax.axis_size("col")
    north, south = lax.rem(me_r + n_r - 1, n_r), lax.rem(me_r + 1, n_r)
    west, east = lax.rem(me_c + n_c - 1, n_c), lax.rem(me_c + 1, n_c)
    others = [(north, me_c), (south, me_c), (me_r, west), (me_r, east),
              (north, west), (north, east), (south, west), (south, east)]
    barrier = pltpu.get_barrier_semaphore()
    for other in others:
        pl.semaphore_signal(barrier, inc=1, device_id=other, device_id_type=MESH)
    pl.semaphore_wait(barrier, len(others))
    up_rows, main_rows, down_rows = pl.ds(0, HALO), pl.ds(HALO, tile), pl.ds(HALO + tile, HALO)
    if first:
        left_main, up_part, down_part = pl.ds(0, tile), pl.ds(0, HALO), pl.ds(tile - HALO, HALO)
        above, below = up_src.at[:, pl.ds(0, HALO), :], down_src.at[:, pl.ds(tile - HALO, HALO), :]
    else:
        left_main, up_part, down_part = main_rows, up_rows, down_rows
        above, below = up_src, down_src
    moves = [
        (left_src.at[:, left_main], from_right.at[:, main_rows], 2),
        (right_src.at[:, left_main], from_left.at[:, main_rows], 3),
        (left_src.at[:, up_part], from_right.at[:, down_rows], 4),
        (right_src.at[:, up_part], from_left.at[:, down_rows], 5),
        (left_src.at[:, down_part], from_right.at[:, up_rows], 6),
        (right_src.at[:, down_part], from_left.at[:, up_rows], 7),
        (above, from_down, 0),
        (below, from_up, 1),
    ]
    copies = []
    for src, dst, k in moves:
        copy = pltpu.make_async_remote_copy(
            src_ref=src, dst_ref=dst, send_sem=send.at[k], recv_sem=recv.at[k],
            device_id=others[k], device_id_type=MESH,
        )
        copy.start()
        copies.append(copy)
    for copy in copies:
        copy.wait()


def exchange(up, down, left, right, tile, first):
    def body(*refs):
        exchange_kernel(0, first, tile, tile, *refs)

    return pl.pallas_call(
        body,
        out_shape=[jax.ShapeDtypeStruct((4, HALO, tile), F32)] * 2
        + [jax.ShapeDtypeStruct((2, tile + 2 * HALO, LANES), F32)] * 2,
        in_specs=[ANY] * 4,
        out_specs=[ANY] * 4,
        scratch_shapes=[pltpu.SemaphoreType.DMA((8,)), pltpu.SemaphoreType.DMA((8,))],
        compiler_params=pltpu.CompilerParams(
            collective_id=0 if first else 1, has_side_effects=True
        ),
        name="halo_in" if first else "halo_out",
    )(up, down, left, right)


def forward(xr, xi, left, right):
    h = xr.shape[0] // 2
    sums = jnp.concatenate([xr[:h] + xr[h:], xi[:h] + xi[h:]], 0).astype(BF16)
    gaps = jnp.concatenate([xr[:h] - xr[h:], xi[:h] - xi[h:]], 0).astype(BF16)
    even = jnp.dot(left[0], sums, preferred_element_type=F32).astype(BF16)
    odd = jnp.dot(left[1], gaps, preferred_element_type=F32).astype(BF16)
    middle = jnp.concatenate(
        [
            jnp.concatenate([even[:h], even[h:]], 1),
            jnp.concatenate([odd[:h], odd[h:]], 1),
        ],
        0,
    )
    out = jnp.dot(middle, right[0], preferred_element_type=F32)
    return out[:, : 2 * h], out[:, 2 * h :]


def inverse(xr, xi, left, right):
    h = xr.shape[0] // 2
    even = jnp.concatenate([xr[:h], xi[:h]], 0).astype(BF16)
    odd = jnp.concatenate([xr[h:], xi[h:]], 0).astype(BF16)
    e = jnp.dot(left[2], even, preferred_element_type=F32)
    o = jnp.dot(left[3], odd, preferred_element_type=F32)
    top, bottom = (e + o).astype(BF16), (e - o).astype(BF16)
    middle = jnp.concatenate(
        [
            jnp.concatenate([top[:h], top[h:]], 1),
            jnp.concatenate([bottom[:h], bottom[h:]], 1),
        ],
        0,
    )
    out = jnp.dot(middle, right[1], preferred_element_type=F32)
    return out[:, : 2 * h], out[:, 2 * h :]


def compute_kernel(
    offsets, objects, up, down, west, east, probe_in, kernel_in, measured_in, left_in, right_in,
    partial, g_up, g_down, g_west, g_east,
    ext, acc, probe, plain, kern, measured, left, right, turned, held, strips, edge, sems,
):
    tile = objects.shape[1]
    width = probe.shape[1]
    h = width // 2
    n_tiles = tile // LANES
    inner = pl.ds(HALO, tile)
    copies = []

    def start(src, dst):
        copy = pltpu.make_async_copy(src, dst, sems.at[len(copies)])
        copy.start()
        copies.append(copy)

    for t in range(n_tiles):
        lanes = pl.ds(t * LANES, LANES)
        start(objects.at[:, :, lanes], ext.at[:, 1 + t, inner, :])
        start(up.at[:, :, lanes], ext.at[:, 1 + t, pl.ds(0, HALO), :])
        start(down.at[:, :, lanes], ext.at[:, 1 + t, pl.ds(HALO + tile, HALO), :])
    start(west, edge.at[0])
    start(east, edge.at[1])
    start(probe_in, probe)
    start(left_in, left)
    start(right_in, right)
    for t in range(width // LANES):
        lanes = pl.ds(t * LANES, LANES)
        start(kernel_in.at[:, :, lanes], plain.at[:, t])
        start(measured_in.at[0, 0, :, :, lanes], measured.at[:, t])
    acc[...] = jnp.zeros_like(acc)
    for copy in copies:
        copy.wait()
    for s in range(2):
        both = edge[0, s]
        ext[2 * s, 0] = pltpu.roll(both, HALF, 1)
        ext[2 * s + 1, 0] = both
        both = edge[1, s]
        ext[2 * s, n_tiles + 1] = both
        ext[2 * s + 1, n_tiles + 1] = pltpu.roll(both, HALF, 1)
    for k in range(2):
        for parity in range(2):
            for t in range(width // LANES):
                kern[k, pl.ds(parity * h, h), pl.ds(t * LANES, LANES)] = plain[
                    k, t, pl.ds(parity, h, stride=2), :
                ]

    def position(p, carry):
        top = offsets[0, 0, p, 0] + HALO
        start_col = offsets[0, 0, p, 1] + LANES
        q = start_col // LANES
        r = start_col - q * LANES
        rows = pl.ds(top, width)
        keep = lane_index((width, LANES)) >= r

        def window(plane):
            first = jnp.where(keep, ext[plane, q, rows, :], ext[plane, q + 2, rows, :])
            return jnp.concatenate([first, ext[plane, q + 1, rows, :]], 1)

        def add(plane, value):
            first = value[:, :LANES]
            acc[plane, q, rows, :] += jnp.where(keep, first, 0.0)
            acc[plane, q + 1, rows, :] += value[:, LANES:]
            acc[plane, q + 2, rows, :] += jnp.where(keep, 0.0, first)

        for k in range(2):
            turned[k] = pltpu.roll(probe[k], r, 1)
        pr, pim = turned[0], turned[1]
        o1r, o1i = window(0), window(1)
        fr, fi = forward(pr * o1r - pim * o1i, pr * o1i + pim * o1r, left, right)
        kr, kim = kern[0], kern[1]
        sr, si = inverse(kr * fr - kim * fi, kr * fi + kim * fr, left, right)
        held[0] = sr
        held[1] = si
        o2r, o2i = window(2), window(3)
        zr, zi = forward(sr * o2r - si * o2i, sr * o2i + si * o2r, left, right)
        amplitude = jnp.concatenate(
            [
                jnp.concatenate(
                    [measured[p, t, pl.ds(k, h, stride=2), :] for t in range(width // LANES)], 1
                )
                for k in range(2)
            ],
            0,
        )
        factor = 1.0 - amplitude * lax.rsqrt(zr * zr + zi * zi + 1.0)
        gr, gi = inverse(zr * factor, zi * factor, left, right)
        sr, si = held[0], held[1]
        add(2, sr * gr + si * gi)
        add(3, sr * gi - si * gr)
        o2r, o2i = window(2), window(3)
        ur, ui = forward(o2r * gr + o2i * gi, o2r * gi - o2i * gr, left, right)
        kr, kim = kern[0], kern[1]
        wr, wi = inverse(kr * ur + kim * ui, kr * ui - kim * ur, left, right)
        pr, pim = turned[0], turned[1]
        add(0, pr * wr + pim * wi)
        add(1, pr * wi - pim * wr)
        return carry

    lax.fori_loop(0, measured.shape[0], position, 0)

    copies = []
    for t in range(n_tiles):
        lanes = pl.ds(t * LANES, LANES)
        start(acc.at[:, 1 + t, pl.ds(0, HALO), :], g_up.at[:, :, lanes])
        start(acc.at[:, 1 + t, pl.ds(HALO + tile, HALO), :], g_down.at[:, :, lanes])
    for s in range(2):
        strips[0, s] = pack_high(acc[2 * s, 0], acc[2 * s + 1, 0])
        strips[1, s] = pack_low(acc[2 * s, n_tiles + 1], acc[2 * s + 1, n_tiles + 1])
    start(strips.at[0], g_west)
    start(strips.at[1], g_east)
    for t in range(n_tiles):
        ext[:, 1 + t, inner, :] = ext[:, 1 + t, inner, :] - RATE * acc[:, 1 + t, inner, :]
        start(ext.at[:, 1 + t, inner, :], partial.at[:, :, pl.ds(t * LANES, LANES)])
    for copy in copies:
        copy.wait()


def compute(objects, halos, probe, kernel, measured, offsets):
    tile, width = objects.shape[1], probe.shape[1]
    n_tiles = tile // LANES
    extent = tile + 2 * HALO
    left, right = tables(width)
    positions = measured.shape[2]
    return pl.pallas_call(
        compute_kernel,
        out_shape=[jax.ShapeDtypeStruct(objects.shape, F32)]
        + [jax.ShapeDtypeStruct((4, HALO, tile), F32)] * 2
        + [jax.ShapeDtypeStruct((2, extent, LANES), F32)] * 2,
        in_specs=[pl.BlockSpec(memory_space=pltpu.SMEM)] + [ANY] * 10,
        out_specs=[ANY] * 5,
        scratch_shapes=[
            pltpu.VMEM((4, n_tiles + 2, extent, LANES), F32),
            pltpu.VMEM((4, n_tiles + 2, extent, LANES), F32),
            pltpu.VMEM(probe.shape, F32),
            pltpu.VMEM((2, width // LANES, width, LANES), F32),
            pltpu.VMEM(probe.shape, F32),
            pltpu.VMEM((positions, width // LANES, width, LANES), F32),
            pltpu.VMEM(left.shape, BF16),
            pltpu.VMEM(right.shape, BF16),
            pltpu.VMEM(probe.shape, F32),
            pltpu.VMEM(probe.shape, F32),
            pltpu.VMEM((2, 2, extent, LANES), F32),
            pltpu.VMEM((2, 2, extent, LANES), F32),
            pltpu.SemaphoreType.DMA((32,)),
        ],
        compiler_params=pltpu.CompilerParams(vmem_limit_bytes=60 * 2**20),
        name="positions",
    )(offsets, objects, *halos, probe, kernel, measured, jnp.asarray(left), jnp.asarray(right))


def border_kernel(partial, up, down, west, east, out, top, bottom, first, last, rows, edge, sems):
    tile = out.shape[1]
    middle = tile - 2 * HALO
    rest = pl.ds(HALO, middle)
    final = pl.ds(out.shape[2] - LANES, LANES)
    copies = []

    def start(src, dst):
        copy = pltpu.make_async_copy(src, dst, sems.at[len(copies)])
        copy.start()
        copies.append(copy)

    targets = [
        (top, out.at[:, pl.ds(0, HALO), :]),
        (bottom, out.at[:, pl.ds(tile - HALO, HALO), :]),
        (first, out.at[:, rest, pl.ds(0, LANES)]),
        (last, out.at[:, rest, final]),
    ]
    for buffer, place in targets:
        start(place, buffer)
    start(up, rows.at[0])
    start(down, rows.at[1])
    start(west, edge.at[0])
    start(east, edge.at[1])
    for copy in copies:
        copy.wait()

    low = lane_index((1, LANES)) < HALF

    def sides(s, begin, count):
        both = edge[0, s, pl.ds(begin, count), :]
        at_first = (jnp.where(low, both, 0.0), jnp.where(low, pltpu.roll(both, HALF, 1), 0.0))
        both = edge[1, s, pl.ds(begin, count), :]
        at_last = (jnp.where(low, 0.0, pltpu.roll(both, HALF, 1)), jnp.where(low, 0.0, both))
        return at_first, at_last

    top[...] = top[...] - RATE * rows[0]
    bottom[...] = bottom[...] - RATE * rows[1]
    for s in range(2):
        at_first, at_last = sides(s, 2 * HALO, middle)
        for k in range(2):
            first[2 * s + k] = first[2 * s + k] - RATE * at_first[k]
            last[2 * s + k] = last[2 * s + k] - RATE * at_last[k]
        for buffer, main, corner in ((top, HALO, 0), (bottom, tile, tile + HALO)):
            mf, ml = sides(s, main, HALO)
            cf, cl = sides(s, corner, HALO)
            for k in range(2):
                p = 2 * s + k
                buffer[p, :, pl.ds(0, LANES)] = buffer[p, :, pl.ds(0, LANES)] - RATE * (mf[k] + cf[k])
                buffer[p, :, final] = buffer[p, :, final] - RATE * (ml[k] + cl[k])
    copies = []
    for buffer, place in targets:
        start(buffer, place)
    for copy in copies:
        copy.wait()


def border(partial, received):
    tile = partial.shape[1]
    extent = tile + 2 * HALO
    return pl.pallas_call(
        border_kernel,
        out_shape=jax.ShapeDtypeStruct(partial.shape, F32),
        in_specs=[ANY] * 5,
        out_specs=ANY,
        scratch_shapes=[
            pltpu.VMEM((4, HALO, tile), F32),
            pltpu.VMEM((4, HALO, tile), F32),
            pltpu.VMEM((4, tile - 2 * HALO, LANES), F32),
            pltpu.VMEM((4, tile - 2 * HALO, LANES), F32),
            pltpu.VMEM((2, 4, HALO, tile), F32),
            pltpu.VMEM((2, 2, extent, LANES), F32),
            pltpu.SemaphoreType.DMA((16,)),
        ],
        input_output_aliases={0: 0},
        name="border",
    )(partial, *received)


def per_device(objects, probe, kernel, measured, offsets):
    tile = objects.shape[1]
    low, high = pack_edges(objects)
    halos = exchange(objects, objects, low, high, tile, True)
    partial, *strips = compute(objects, halos, probe, kernel, measured, offsets)
    received = exchange(*strips, tile, False)
    return border(partial, received)


def solution(mesh):
    return jax.shard_map(
        per_device,
        mesh=mesh,
        in_specs=(
            P(None, "row", "col"),
            P(),
            P(),
            P("row", "col", None, None, None),
            P("row", "col", None, None),
        ),
        out_specs=P(None, "row", "col"),
        check_vma=False,
    )
```

```python
import functools

import jax
import jax.numpy as jnp
import numpy as np
from jax import lax
from jax.experimental import pallas as pl
from jax.experimental.pallas import tpu as pltpu
from jax.sharding import PartitionSpec as P

HALO = 64
RATE = 0.5
LANES = 128
HALF = 64
MESH = pl.DeviceIdType.MESH
BF16 = jnp.bfloat16
F32 = jnp.float32
ANY = pl.BlockSpec(memory_space=pl.ANY)


@functools.cache
def tables(width):
    index = np.arange(width)
    angle = 2.0 * np.pi / width * (index[:, None] * index[None, :] % width)
    norm = 1.0 / np.sqrt(width)
    cosine = (np.cos(angle) * norm).astype(np.float32)
    sine = (np.sin(angle) * norm).astype(np.float32)

    def left(r, i):
        return np.concatenate(
            [np.concatenate([r, -i], 1), np.concatenate([i, r], 1)], 0
        ).astype(BF16)

    def right(r, i):
        return np.concatenate(
            [np.concatenate([r, i], 1), np.concatenate([-i, r], 1)], 0
        ).astype(BF16)

    h = width // 2
    split = []
    for parity in (0, 1):
        split.append(left(cosine[parity::2, :h], -sine[parity::2, :h]))
    for parity in (0, 1):
        split.append(left(cosine[:h, parity::2], sine[:h, parity::2]))
    return np.stack(split), np.stack([right(cosine, -sine), right(cosine, sine)])


def lane_index(shape):
    return lax.broadcasted_iota(jnp.int32, shape, len(shape) - 1)


def pack_high(re, im):
    return jnp.where(lane_index(re.shape) < HALF, pltpu.roll(re, HALF, re.ndim - 1), im)


def pack_low(re, im):
    return jnp.where(lane_index(re.shape) < HALF, re, pltpu.roll(im, HALF, im.ndim - 1))


def forward(xr, xi, left, right):
    h = xr.shape[0] // 2
    sums = jnp.concatenate([xr[:h] + xr[h:], xi[:h] + xi[h:]], 0).astype(BF16)
    gaps = jnp.concatenate([xr[:h] - xr[h:], xi[:h] - xi[h:]], 0).astype(BF16)
    even = jnp.dot(left[0], sums, preferred_element_type=F32).astype(BF16)
    odd = jnp.dot(left[1], gaps, preferred_element_type=F32).astype(BF16)
    middle = jnp.concatenate(
        [
            jnp.concatenate([even[:h], even[h:]], 1),
            jnp.concatenate([odd[:h], odd[h:]], 1),
        ],
        0,
    )
    out = jnp.dot(middle, right[0], preferred_element_type=F32)
    return out[:, : 2 * h], out[:, 2 * h :]


def inverse(xr, xi, left, right):
    h = xr.shape[0] // 2
    even = jnp.concatenate([xr[:h], xi[:h]], 0).astype(BF16)
    odd = jnp.concatenate([xr[h:], xi[h:]], 0).astype(BF16)
    e = jnp.dot(left[2], even, preferred_element_type=F32)
    o = jnp.dot(left[3], odd, preferred_element_type=F32)
    top, bottom = (e + o).astype(BF16), (e - o).astype(BF16)
    middle = jnp.concatenate(
        [
            jnp.concatenate([top[:h], top[h:]], 1),
            jnp.concatenate([bottom[:h], bottom[h:]], 1),
        ],
        0,
    )
    out = jnp.dot(middle, right[1], preferred_element_type=F32)
    return out[:, : 2 * h], out[:, 2 * h :]


def step_kernel(
    offsets, objects, probe_in, kernel_in, measured_in, left_in, right_in,
    out,
    ext1, ext2, probe, turned, plain, kern, measured, left, right, held, pieces,
    strips, edge1, edge2, g_rows1, g_rows2, g_cols1, g_cols2, r_rows1, r_rows2, r_cols1, r_cols2,
    load_sems, send, recv, out_sems,
):
    tile = objects.shape[1]
    width = probe.shape[1]
    h = width // 2
    n_tiles = tile // LANES
    positions = measured.shape[0]
    extent = tile + 2 * HALO
    gap = extent - width
    inner = pl.ds(HALO, tile)
    up_rows, down_rows = pl.ds(0, HALO), pl.ds(HALO + tile, HALO)
    first_rows, last_rows = pl.ds(HALO, HALO), pl.ds(tile, HALO)
    body_tiles = pl.ds(1, n_tiles)
    ext = (ext1, ext2)
    edge = (edge1, edge2)
    g_rows, g_cols = (g_rows1, g_rows2), (g_cols1, g_cols2)
    r_rows, r_cols = (r_rows1, r_rows2), (r_cols1, r_cols2)

    me_r, me_c = lax.axis_index("row"), lax.axis_index("col")
    n_r, n_c = lax.axis_size("row"), lax.axis_size("col")
    north, south = lax.rem(me_r + n_r - 1, n_r), lax.rem(me_r + 1, n_r)
    west, east = lax.rem(me_c + n_c - 1, n_c), lax.rem(me_c + 1, n_c)
    others = [(north, me_c), (south, me_c), (me_r, west), (me_r, east),
              (north, west), (north, east), (south, west), (south, east)]
    barrier = pltpu.get_barrier_semaphore()
    for other in others:
        pl.semaphore_signal(barrier, inc=1, device_id=other, device_id_type=MESH)

    loads = []

    def load(src, dst):
        copy = pltpu.make_async_copy(src, dst, load_sems.at[len(loads)])
        copy.start()
        loads.append(copy)

    for s in range(2):
        for t in range(n_tiles):
            load(objects.at[pl.ds(2 * s, 2), :, pl.ds(t * LANES, LANES)], ext[s].at[:, 1 + t, inner, :])
    n_object = len(loads)
    load(probe_in, probe)
    for t in range(width // LANES):
        load(kernel_in.at[:, :, pl.ds(t * LANES, LANES)], plain.at[:, t])
    load(left_in, left)
    load(right_in, right)
    for t in range(width // LANES):
        load(measured_in.at[0, 0, :, :, pl.ds(t * LANES, LANES)], measured.at[:, t])

    def exchange(phase, above, below, to_west, to_east, base, from_up, from_down, from_west, from_east):
        main = pl.ds(base, tile)
        upper = pl.ds(0, HALO)
        lower = pl.ds(base + tile + base - HALO, HALO)
        landed = inner
        moves = [
            (to_west.at[main], from_east.at[landed], 2),
            (to_east.at[main], from_west.at[landed], 3),
            (to_west.at[upper], from_east.at[down_rows], 4),
            (to_east.at[upper], from_west.at[down_rows], 5),
            (to_west.at[lower], from_east.at[up_rows], 6),
            (to_east.at[lower], from_west.at[up_rows], 7),
            (above, from_down, 0),
            (below, from_up, 1),
        ]
        copies = []
        for src, dst, k in moves:
            copy = pltpu.make_async_remote_copy(
                src_ref=src, dst_ref=dst, send_sem=send.at[phase, k], recv_sem=recv.at[phase, k],
                device_id=others[k], device_id_type=MESH,
            )
            copy.start()
            copies.append(copy)
        return copies

    def send_halo(s):
        e = ext[s]
        return exchange(
            s,
            e.at[:, body_tiles, first_rows, :], e.at[:, body_tiles, last_rows, :],
            strips.at[s, 0], strips.at[s, 1], 0,
            e.at[:, body_tiles, up_rows, :], e.at[:, body_tiles, down_rows, :],
            edge[s].at[0], edge[s].at[1],
        )

    def send_gradient(s):
        g, r = g_rows[s], r_rows[s]
        c, d = g_cols[s], r_cols[s]
        return exchange(
            2 + s, g.at[0], g.at[1], c.at[0], c.at[1], HALO, r.at[0], r.at[1], d.at[0], d.at[1]
        )

    for copy in loads[:n_object]:
        copy.wait()
    for s in range(2):
        strips[s, 0] = pack_low(ext[s][0, 1, inner, :], ext[s][1, 1, inner, :])
        strips[s, 1] = pack_high(ext[s][0, n_tiles, inner, :], ext[s][1, n_tiles, inner, :])
    pl.semaphore_wait(barrier, len(others))
    halo1 = send_halo(0)

    for copy in loads[n_object:]:
        copy.wait()
    pieces[...] = jnp.zeros_like(pieces)
    for k in range(2):
        for parity in range(2):
            for t in range(width // LANES):
                kern[k, pl.ds(parity * h, h), pl.ds(t * LANES, LANES)] = plain[
                    k, t, pl.ds(parity, h, stride=2), :
                ]

    def where_of(p):
        top = offsets[0, 0, p, 0] + HALO
        start = offsets[0, 0, p, 1] + LANES
        q = start // LANES
        return top, start, q, start - q * LANES

    def turn(p, carry):
        r = where_of(p)[3]
        for k in range(2):
            turned[p, k] = pltpu.roll(probe[k], r, 1)
        return carry

    lax.fori_loop(0, positions, turn, 0)

    def unpack_halo(s):
        both = edge[s][0]
        ext[s][0, 0] = pltpu.roll(both, HALF, 1)
        ext[s][1, 0] = both
        both = edge[s][1]
        ext[s][0, n_tiles + 1] = both
        ext[s][1, n_tiles + 1] = pltpu.roll(both, HALF, 1)

    def window(s, plane, p):
        top, _, q, r = where_of(p)
        rows = pl.ds(top, width)
        keep = lane_index((width, LANES)) >= r
        first = jnp.where(keep, ext[s][plane, q, rows, :], ext[s][plane, q + 2, rows, :])
        return jnp.concatenate([first, ext[s][plane, q + 1, rows, :]], 1)

    def put(p, c, value):
        rows = pl.ds(gap + p * extent, width)
        pieces[c, 0, rows, :] = value[:, :LANES]
        pieces[c, 1, rows, :] = value[:, LANES:]

    for copy in halo1:
        copy.wait()
    halo2 = send_halo(1)
    unpack_halo(0)

    def stage_a(p, carry):
        pr, pim = turned[p, 0], turned[p, 1]
        o1r, o1i = window(0, 0, p), window(0, 1, p)
        fr, fi = forward(pr * o1r - pim * o1i, pr * o1i + pim * o1r, left, right)
        kr, kim = kern[0], kern[1]
        sr, si = inverse(kr * fr - kim * fi, kr * fi + kim * fr, left, right)
        held[p, 0] = sr
        held[p, 1] = si
        return carry

    lax.fori_loop(0, positions, stage_a, 0)

    for copy in halo2:
        copy.wait()
    unpack_halo(1)

    def stage_b(p, carry):
        sr, si = held[p, 0], held[p, 1]
        o2r, o2i = window(1, 0, p), window(1, 1, p)
        zr, zi = forward(sr * o2r - si * o2i, sr * o2i + si * o2r, left, right)
        amplitude = jnp.concatenate(
            [
                jnp.concatenate(
                    [measured[p, t, pl.ds(k, h, stride=2), :] for t in range(width // LANES)], 1
                )
                for k in range(2)
            ],
            0,
        )
        factor = 1.0 - amplitude * lax.rsqrt(zr * zr + zi * zi + 1.0)
        gr, gi = inverse(zr * factor, zi * factor, left, right)
        sr, si = held[p, 0], held[p, 1]
        put(p, 0, sr * gr + si * gi)
        put(p, 1, sr * gi - si * gr)
        o2r, o2i = window(1, 0, p), window(1, 1, p)
        held[p, 0] = o2r * gr + o2i * gi
        held[p, 1] = o2r * gi - o2i * gr
        return carry

    lax.fori_loop(0, positions, stage_b, 0)

    def gather(c, t, row, count):
        total = jnp.zeros((count, LANES), F32)
        lane = lane_index((count, LANES)) + t * LANES
        for p in range(positions):
            top, start, q, _ = where_of(p)
            value = pieces[c, (t + 8 - q) % 2, pl.ds(gap + p * extent - top + row, count), :]
            total = total + jnp.where((lane >= start) & (lane < start + width), value, 0.0)
        return total

    def gather_borders(s):
        def sides(i, carry):
            row = pl.multiple_of(i * HALO, HALO)
            rows = pl.ds(row, HALO)
            g_cols[s][0, rows, :] = pack_high(gather(0, 0, row, HALO), gather(1, 0, row, HALO))
            g_cols[s][1, rows, :] = pack_low(
                gather(0, n_tiles + 1, row, HALO), gather(1, n_tiles + 1, row, HALO)
            )
            return carry

        lax.fori_loop(0, extent // HALO, sides, 0)

        def ends(i, carry):
            for c in range(2):
                g_rows[s][0, c, i] = gather(c, 1 + i, 0, HALO)
                g_rows[s][1, c, i] = gather(c, 1 + i, HALO + tile, HALO)
            return carry

        lax.fori_loop(0, n_tiles, ends, 0)

    def gather_inner(s):
        def chunk(i, carry):
            row = pl.multiple_of(HALO + i * HALO, HALO)
            rows = pl.ds(row, HALO)
            for c in range(2):
                for t in range(1, n_tiles + 1):
                    ext[s][c, t, rows, :] = ext[s][c, t, rows, :] - RATE * gather(c, t, row, HALO)
            return carry

        lax.fori_loop(0, tile // HALO, chunk, 0)

    def add_borders(s):
        e = ext[s]
        for t in range(n_tiles):
            for c in range(2):
                e[c, 1 + t, first_rows, :] = e[c, 1 + t, first_rows, :] - RATE * r_rows[s][0, c, t]
                e[c, 1 + t, last_rows, :] = e[c, 1 + t, last_rows, :] - RATE * r_rows[s][1, c, t]
        for rows, source in ((inner, inner), (first_rows, up_rows), (last_rows, down_rows)):
            both = r_cols[s][0, source, :]
            low = lane_index(both.shape) < HALF
            swapped = pltpu.roll(both, HALF, 1)
            e[0, 1, rows, :] = e[0, 1, rows, :] - RATE * jnp.where(low, both, 0.0)
            e[1, 1, rows, :] = e[1, 1, rows, :] - RATE * jnp.where(low, swapped, 0.0)
            both = r_cols[s][1, source, :]
            swapped = pltpu.roll(both, HALF, 1)
            e[0, n_tiles, rows, :] = e[0, n_tiles, rows, :] - RATE * jnp.where(low, 0.0, swapped)
            e[1, n_tiles, rows, :] = e[1, n_tiles, rows, :] - RATE * jnp.where(low, 0.0, both)

    def store(s):
        copies = []
        for t in range(n_tiles):
            copy = pltpu.make_async_copy(
                ext[s].at[:, 1 + t, inner, :],
                out.at[pl.ds(2 * s, 2), :, pl.ds(t * LANES, LANES)],
                out_sems.at[s, t],
            )
            copy.start()
            copies.append(copy)
        return copies

    gather_borders(1)
    sent2 = send_gradient(1)
    gather_inner(1)

    def stage_c(p, carry):
        ur, ui = forward(held[p, 0], held[p, 1], left, right)
        kr, kim = kern[0], kern[1]
        wr, wi = inverse(kr * ur + kim * ui, kr * ui - kim * ur, left, right)
        pr, pim = turned[p, 0], turned[p, 1]
        put(p, 0, pr * wr + pim * wi)
        put(p, 1, pr * wi - pim * wr)
        return carry

    lax.fori_loop(0, positions, stage_c, 0)

    gather_borders(0)
    for copy in sent2:
        copy.wait()
    sent1 = send_gradient(0)
    gather_inner(0)
    add_borders(1)
    stored = store(1)
    for copy in sent1:
        copy.wait()
    add_borders(0)
    stored = stored + store(0)
    for copy in stored:
        copy.wait()


def per_device(objects, probe, kernel, measured, offsets):
    tile, width = objects.shape[1], probe.shape[1]
    n_tiles = tile // LANES
    extent = tile + 2 * HALO
    left, right = tables(width)
    positions = measured.shape[2]
    ext = pltpu.VMEM((2, n_tiles + 2, extent, LANES), F32)
    planes = pltpu.VMEM((positions, 2, width, width), F32)
    cols = pltpu.VMEM((2, extent, LANES), F32)
    rows = pltpu.VMEM((2, 2, n_tiles, HALO, LANES), F32)
    dma = pltpu.SemaphoreType.DMA
    return pl.pallas_call(
        step_kernel,
        out_shape=jax.ShapeDtypeStruct(objects.shape, F32),
        in_specs=[pl.BlockSpec(memory_space=pltpu.SMEM)] + [ANY] * 6,
        out_specs=ANY,
        scratch_shapes=[
            ext,
            ext,
            pltpu.VMEM(probe.shape, F32),
            planes,
            pltpu.VMEM((2, width // LANES, width, LANES), F32),
            pltpu.VMEM(probe.shape, F32),
            pltpu.VMEM((positions, width // LANES, width, LANES), F32),
            pltpu.VMEM(left.shape, BF16),
            pltpu.VMEM(right.shape, BF16),
            planes,
            pltpu.VMEM((2, 2, positions * extent + extent - width, LANES), F32),
            pltpu.VMEM((2, 2, tile, LANES), F32),
            cols, cols, rows, rows, cols, cols, rows, rows, cols, cols,
            dma((24,)), dma((4, 8)), dma((4, 8)), dma((2, n_tiles)),
        ],
        compiler_params=pltpu.CompilerParams(
            vmem_limit_bytes=63 * 2**20, collective_id=0, has_side_effects=True
        ),
        name="step",
    )(offsets, objects, probe, kernel, measured, jnp.asarray(left), jnp.asarray(right))


def solution(mesh):
    return jax.shard_map(
        per_device,
        mesh=mesh,
        in_specs=(
            P(None, "row", "col"),
            P(),
            P(),
            P("row", "col", None, None, None),
            P("row", "col", None, None),
        ),
        out_specs=P(None, "row", "col"),
        check_vma=False,
    )
```

```python
import functools

import jax
import jax.numpy as jnp
import numpy as np
from jax import lax
from jax.experimental import pallas as pl
from jax.experimental.pallas import tpu as pltpu
from jax.sharding import PartitionSpec as P

HALO = 64
RATE = 0.5
LANES = 128
HALF = 64
MESH = pl.DeviceIdType.MESH
BF16 = jnp.bfloat16
F32 = jnp.float32
ANY = pl.BlockSpec(memory_space=pl.ANY)


@functools.cache
def tables(width):
    index = np.arange(width)
    angle = 2.0 * np.pi / width * (index[:, None] * index[None, :] % width)
    norm = 1.0 / np.sqrt(width)
    cosine = (np.cos(angle) * norm).astype(np.float32)
    sine = (np.sin(angle) * norm).astype(np.float32)

    def left(r, i):
        return np.concatenate(
            [np.concatenate([r, -i], 1), np.concatenate([i, r], 1)], 0
        ).astype(BF16)

    def right(r, i):
        return np.concatenate(
            [np.concatenate([r, i], 1), np.concatenate([-i, r], 1)], 0
        ).astype(BF16)

    h = width // 2
    split = []
    for parity in (0, 1):
        split.append(left(cosine[parity::2, :h], -sine[parity::2, :h]))
    for parity in (0, 1):
        split.append(left(cosine[:h, parity::2], sine[:h, parity::2]))
    return np.stack(split), np.stack([right(cosine, -sine), right(cosine, sine)])


def lane_index(shape):
    return lax.broadcasted_iota(jnp.int32, shape, len(shape) - 1)


def pack_high(re, im):
    return jnp.where(lane_index(re.shape) < HALF, pltpu.roll(re, HALF, re.ndim - 1), im)


def pack_low(re, im):
    return jnp.where(lane_index(re.shape) < HALF, re, pltpu.roll(im, HALF, im.ndim - 1))


def forward(xr, xi, left, right):
    h = xr.shape[0] // 2
    sums = jnp.concatenate([xr[:h] + xr[h:], xi[:h] + xi[h:]], 0).astype(BF16)
    gaps = jnp.concatenate([xr[:h] - xr[h:], xi[:h] - xi[h:]], 0).astype(BF16)
    even = jnp.dot(left[0], sums, preferred_element_type=F32).astype(BF16)
    odd = jnp.dot(left[1], gaps, preferred_element_type=F32).astype(BF16)
    middle = jnp.concatenate(
        [
            jnp.concatenate([even[:h], even[h:]], 1),
            jnp.concatenate([odd[:h], odd[h:]], 1),
        ],
        0,
    )
    out = jnp.dot(middle, right[0], preferred_element_type=F32)
    return out[:, : 2 * h], out[:, 2 * h :]


def inverse(xr, xi, left, right):
    h = xr.shape[0] // 2
    even = jnp.concatenate([xr[:h], xi[:h]], 0).astype(BF16)
    odd = jnp.concatenate([xr[h:], xi[h:]], 0).astype(BF16)
    e = jnp.dot(left[2], even, preferred_element_type=F32)
    o = jnp.dot(left[3], odd, preferred_element_type=F32)
    top, bottom = (e + o).astype(BF16), (e - o).astype(BF16)
    middle = jnp.concatenate(
        [
            jnp.concatenate([top[:h], top[h:]], 1),
            jnp.concatenate([bottom[:h], bottom[h:]], 1),
        ],
        0,
    )
    out = jnp.dot(middle, right[1], preferred_element_type=F32)
    return out[:, : 2 * h], out[:, 2 * h :]


def step_kernel(
    offsets, objects, probe_in, kernel_in, measured_in, left_in, right_in,
    out,
    ext1, ext2, probe, turned, plain, kern, measured, left, right, held, pieces,
    strips, edge1, edge2, g_rows1, g_rows2, g_cols1, g_cols2, r_rows1, r_rows2, r_cols1, r_cols2,
    load_sems, send, recv,
):
    tile = objects.shape[1]
    width = probe.shape[1]
    h = width // 2
    n_tiles = tile // LANES
    positions = measured.shape[0]
    extent = tile + 2 * HALO
    gap = extent - width
    inner = pl.ds(HALO, tile)
    up_rows, down_rows = pl.ds(0, HALO), pl.ds(HALO + tile, HALO)
    first_rows, last_rows = pl.ds(HALO, HALO), pl.ds(tile, HALO)
    body_tiles = pl.ds(1, n_tiles)
    ext = (ext1, ext2)
    edge = (edge1, edge2)
    g_rows, g_cols = (g_rows1, g_rows2), (g_cols1, g_cols2)
    r_rows, r_cols = (r_rows1, r_rows2), (r_cols1, r_cols2)

    me_r, me_c = lax.axis_index("row"), lax.axis_index("col")
    n_r, n_c = lax.axis_size("row"), lax.axis_size("col")
    north, south = lax.rem(me_r + n_r - 1, n_r), lax.rem(me_r + 1, n_r)
    west, east = lax.rem(me_c + n_c - 1, n_c), lax.rem(me_c + 1, n_c)
    has_n, has_s, has_w, has_e = me_r > 0, me_r < n_r - 1, me_c > 0, me_c < n_c - 1
    others = [(north, me_c), (south, me_c), (me_r, west), (me_r, east),
              (north, west), (north, east), (south, west), (south, east)]
    here = [has_n, has_s, has_w, has_e, has_n & has_w, has_n & has_e, has_s & has_w, has_s & has_e]
    opposite = [1, 0, 3, 2, 7, 6, 5, 4]
    for ref in (r_rows1, r_rows2, r_cols1, r_cols2):
        ref[...] = jnp.zeros_like(ref)
    barrier = pltpu.get_barrier_semaphore()
    neighbours = 0
    for other, there in zip(others, here):
        neighbours = neighbours + there.astype(jnp.int32)

        @pl.when(there)
        def _():
            pl.semaphore_signal(barrier, inc=1, device_id=other, device_id_type=MESH)

    loads = []

    def load(src, dst):
        copy = pltpu.make_async_copy(src, dst, load_sems.at[len(loads)])
        copy.start()
        loads.append(copy)

    for s in range(2):
        for t in range(n_tiles):
            load(objects.at[pl.ds(2 * s, 2), :, pl.ds(t * LANES, LANES)], ext[s].at[:, 1 + t, inner, :])
    load(probe_in, probe)
    for t in range(width // LANES):
        load(kernel_in.at[:, :, pl.ds(t * LANES, LANES)], plain.at[:, t])
    load(left_in, left)
    load(right_in, right)
    for t in range(width // LANES):
        load(measured_in.at[0, 0, :, :, pl.ds(t * LANES, LANES)], measured.at[:, t])

    def exchange(phase, above, below, to_west, to_east, base, from_up, from_down, from_west, from_east):
        main = pl.ds(base, tile)
        upper = pl.ds(0, HALO)
        lower = pl.ds(base + tile + base - HALO, HALO)
        landed = inner
        moves = [
            (to_west.at[main], from_east.at[landed], 2),
            (to_east.at[main], from_west.at[landed], 3),
            (to_west.at[upper], from_east.at[down_rows], 4),
            (to_east.at[upper], from_west.at[down_rows], 5),
            (to_west.at[lower], from_east.at[up_rows], 6),
            (to_east.at[lower], from_west.at[up_rows], 7),
            (above, from_down, 0),
            (below, from_up, 1),
        ]
        copies = []
        for src, dst, k in moves:
            copy = pltpu.make_async_remote_copy(
                src_ref=src, dst_ref=dst, send_sem=send.at[phase, k], recv_sem=recv.at[phase, k],
                device_id=others[k], device_id_type=MESH,
            )
            pl.when(here[k])(copy.start)
            copies.append((copy, k))
        return copies

    def finish(copies):
        for copy, k in copies:
            pl.when(here[k])(copy.wait_send)
            pl.when(here[opposite[k]])(copy.wait_recv)

    def send_halo(s):
        e = ext[s]
        return exchange(
            s,
            e.at[:, body_tiles, first_rows, :], e.at[:, body_tiles, last_rows, :],
            strips.at[s, 0], strips.at[s, 1], 0,
            e.at[:, body_tiles, up_rows, :], e.at[:, body_tiles, down_rows, :],
            edge[s].at[0], edge[s].at[1],
        )

    def send_gradient(s):
        g, r = g_rows[s], r_rows[s]
        c, d = g_cols[s], r_cols[s]
        return exchange(
            2 + s, g.at[0], g.at[1], c.at[0], c.at[1], HALO, r.at[0], r.at[1], d.at[0], d.at[1]
        )

    for copy in loads[:n_tiles]:
        copy.wait()

    def pack(s):
        strips[s, 0] = pack_low(ext[s][0, 1, inner, :], ext[s][1, 1, inner, :])
        strips[s, 1] = pack_high(ext[s][0, n_tiles, inner, :], ext[s][1, n_tiles, inner, :])
    pack(0)
    pl.semaphore_wait(barrier, neighbours)
    halo1 = send_halo(0)

    for copy in loads[n_tiles:]:
        copy.wait()
    pack(1)
    def clear(i, carry):
        rows = pl.ds(pl.multiple_of(i * extent, LANES), gap)
        pieces[:, :, rows, :] = jnp.zeros((2, 3, gap, LANES), F32)
        return carry

    lax.fori_loop(0, positions + 1, clear, 0)
    for k in range(2):
        for parity in range(2):
            for t in range(width // LANES):
                kern[k, pl.ds(parity * h, h), pl.ds(t * LANES, LANES)] = plain[
                    k, t, pl.ds(parity, h, stride=2), :
                ]

    def where_of(p):
        top = offsets[0, 0, 0, p] + HALO
        start = offsets[0, 0, 1, p] + LANES
        q = start // LANES
        return top, q, start - q * LANES

    def turn(p, carry):
        r = where_of(p)[2]
        for k in range(2):
            turned[p, k] = pltpu.roll(probe[k], r, 1)
        return carry

    lax.fori_loop(0, positions, turn, 0)

    def unpack_halo(s):
        both = edge[s][0]
        ext[s][0, 0] = pltpu.roll(both, HALF, 1)
        ext[s][1, 0] = both
        both = edge[s][1]
        ext[s][0, n_tiles + 1] = both
        ext[s][1, n_tiles + 1] = pltpu.roll(both, HALF, 1)

    def window(s, plane, p):
        top, q, r = where_of(p)
        rows = pl.ds(top, width)
        keep = lane_index((width, LANES)) >= r
        first = jnp.where(keep, ext[s][plane, q, rows, :], ext[s][plane, q + 2, rows, :])
        return jnp.concatenate([first, ext[s][plane, q + 1, rows, :]], 1)

    def put(p, c, value):
        rows = pl.ds(gap + p * extent, width)
        keep = lane_index((width, LANES)) >= where_of(p)[2]
        first = value[:, :LANES]
        pieces[c, 0, rows, :] = jnp.where(keep, first, 0.0)
        pieces[c, 1, rows, :] = value[:, LANES:]
        pieces[c, 2, rows, :] = jnp.where(keep, 0.0, first)

    finish(halo1)
    halo2 = send_halo(1)
    unpack_halo(0)

    def stage_a(p, carry):
        pr, pim = turned[p, 0], turned[p, 1]
        o1r, o1i = window(0, 0, p), window(0, 1, p)
        fr, fi = forward(pr * o1r - pim * o1i, pr * o1i + pim * o1r, left, right)
        kr, kim = kern[0], kern[1]
        sr, si = inverse(kr * fr - kim * fi, kr * fi + kim * fr, left, right)
        held[p, 0] = sr
        held[p, 1] = si
        return carry

    lax.fori_loop(0, positions, stage_a, 0, unroll=3)

    finish(halo2)
    unpack_halo(1)

    def stage_b(p, carry):
        sr, si = held[p, 0], held[p, 1]
        o2r, o2i = window(1, 0, p), window(1, 1, p)
        zr, zi = forward(sr * o2r - si * o2i, sr * o2i + si * o2r, left, right)
        amplitude = jnp.concatenate(
            [
                jnp.concatenate(
                    [measured[p, t, pl.ds(k, h, stride=2), :] for t in range(width // LANES)], 1
                )
                for k in range(2)
            ],
            0,
        )
        factor = 1.0 - amplitude * lax.rsqrt(zr * zr + zi * zi + 1.0)
        gr, gi = inverse(zr * factor, zi * factor, left, right)
        sr, si = held[p, 0], held[p, 1]
        put(p, 0, sr * gr + si * gi)
        put(p, 1, sr * gi - si * gr)
        o2r, o2i = window(1, 0, p), window(1, 1, p)
        held[p, 0] = o2r * gr + o2i * gi
        held[p, 1] = o2r * gi - o2i * gr
        return carry

    lax.fori_loop(0, positions, stage_b, 0, unroll=3)

    def gather(t, row, count):
        totals = [jnp.zeros((count, LANES), F32)] * 2
        for p in range(positions):
            top, q, _ = spots[p]
            inside = (t >= q) & (t <= q + 2)
            slot = jnp.where(inside, t - q, 0)
            rows = pl.ds(jnp.where(inside, gap + p * extent - top + row, 0), count)
            totals = [totals[c] + pieces[c, slot, rows, :] for c in range(2)]
        return totals

    def gather_borders(s):
        def sides(i, carry):
            row = pl.multiple_of(i * HALO, HALO)
            rows = pl.ds(row, HALO)
            g_cols[s][0, rows, :] = pack_high(*gather(0, row, HALO))
            g_cols[s][1, rows, :] = pack_low(*gather(n_tiles + 1, row, HALO))
            return carry

        lax.fori_loop(0, extent // HALO, sides, 0)

        def ends(i, carry):
            for k in range(2):
                totals = gather(1 + i, k * (HALO + tile), HALO)
                for c in range(2):
                    g_rows[s][k, c, i] = totals[c]
            return carry

        lax.fori_loop(0, n_tiles, ends, 0)

    def gather_inner(s):
        def chunk(i, carry):
            row = pl.multiple_of(i * HALO, HALO)
            for t in range(n_tiles):
                totals = gather(t + 1, row + HALO, HALO)
                for c in range(2):
                    out[2 * s + c, pl.ds(row, HALO), pl.ds(t * LANES, LANES)] = (
                        ext[s][c, t + 1, pl.ds(row + HALO, HALO), :] - RATE * totals[c]
                    )
            return carry

        lax.fori_loop(0, tile // HALO, chunk, 0)

    def subtract(plane, rows, t, value):
        lanes = pl.ds(t * LANES, LANES)
        out[plane, rows, lanes] = out[plane, rows, lanes] - RATE * value

    def add_borders(s):
        begin, end = pl.ds(0, HALO), pl.ds(tile - HALO, HALO)
        for t in range(n_tiles):
            for c in range(2):
                subtract(2 * s + c, begin, t, r_rows[s][0, c, t])
                subtract(2 * s + c, end, t, r_rows[s][1, c, t])
        for rows, source in ((pl.ds(0, tile), inner), (begin, up_rows), (end, down_rows)):
            both = r_cols[s][0, source, :]
            low = lane_index(both.shape) < HALF
            subtract(2 * s, rows, 0, jnp.where(low, both, 0.0))
            subtract(2 * s + 1, rows, 0, jnp.where(low, pltpu.roll(both, HALF, 1), 0.0))
            both = r_cols[s][1, source, :]
            subtract(2 * s, rows, n_tiles - 1, jnp.where(low, 0.0, pltpu.roll(both, HALF, 1)))
            subtract(2 * s + 1, rows, n_tiles - 1, jnp.where(low, 0.0, both))

    spots = [where_of(p) for p in range(positions)]
    gather_borders(1)
    sent2 = send_gradient(1)
    gather_inner(1)

    def stage_c(p, carry):
        ur, ui = forward(held[p, 0], held[p, 1], left, right)
        kr, kim = kern[0], kern[1]
        wr, wi = inverse(kr * ur + kim * ui, kr * ui - kim * ur, left, right)
        pr, pim = turned[p, 0], turned[p, 1]
        put(p, 0, pr * wr + pim * wi)
        put(p, 1, pr * wi - pim * wr)
        return carry

    lax.fori_loop(0, positions, stage_c, 0, unroll=3)

    gather_borders(0)
    finish(sent2)
    sent1 = send_gradient(0)
    gather_inner(0)
    add_borders(1)
    finish(sent1)
    add_borders(0)


def per_device(objects, probe, kernel, measured, offsets):
    tile, width = objects.shape[1], probe.shape[1]
    n_tiles = tile // LANES
    extent = tile + 2 * HALO
    left, right = tables(width)
    positions = measured.shape[2]
    ext = pltpu.VMEM((2, n_tiles + 2, extent, LANES), F32)
    planes = pltpu.VMEM((positions, 2, width, width), F32)
    cols = pltpu.VMEM((2, extent, LANES), F32)
    rows = pltpu.VMEM((2, 2, n_tiles, HALO, LANES), F32)
    dma = pltpu.SemaphoreType.DMA
    return pl.pallas_call(
        step_kernel,
        out_shape=pltpu.VMEM(objects.shape, F32),
        in_specs=[pl.BlockSpec(memory_space=pltpu.SMEM)] + [ANY] * 6,
        out_specs=pl.BlockSpec(memory_space=pltpu.VMEM),
        scratch_shapes=[
            ext,
            ext,
            pltpu.VMEM(probe.shape, F32),
            planes,
            pltpu.VMEM((2, width // LANES, width, LANES), F32),
            pltpu.VMEM(probe.shape, F32),
            pltpu.VMEM((positions, width // LANES, width, LANES), F32),
            pltpu.VMEM(left.shape, BF16),
            pltpu.VMEM(right.shape, BF16),
            planes,
            pltpu.VMEM((2, 3, positions * extent + extent - width, LANES), F32),
            pltpu.VMEM((2, 2, tile, LANES), F32),
            cols, cols, rows, rows, cols, cols, rows, rows, cols, cols,
            dma((24,)), dma((4, 8)), dma((4, 8)),
        ],
        compiler_params=pltpu.CompilerParams(
            vmem_limit_bytes=58 * 2**20, collective_id=0, has_side_effects=True
        ),
        name="step",
    )(jnp.swapaxes(offsets, 2, 3), objects, probe, kernel, measured, jnp.asarray(left), jnp.asarray(right))


def solution(mesh):
    return jax.shard_map(
        per_device,
        mesh=mesh,
        in_specs=(
            P(None, "row", "col"),
            P(),
            P(),
            P("row", "col", None, None, None),
            P("row", "col", None, None),
        ),
        out_specs=P(None, "row", "col"),
        check_vma=False,
    )
```

```python
import functools

import jax
import jax.numpy as jnp
import numpy as np
from jax import lax
from jax.experimental import pallas as pl
from jax.experimental.pallas import tpu as pltpu
from jax.sharding import PartitionSpec as P

HALO = 64
RATE = 0.5
LANES = 128
HALF = 64
MESH = pl.DeviceIdType.MESH
BF16 = jnp.bfloat16
F32 = jnp.float32
ANY = pl.BlockSpec(memory_space=pl.ANY)


@functools.cache
def tables(width):
    index = np.arange(width)
    angle = 2.0 * np.pi / width * (index[:, None] * index[None, :] % width)
    norm = 1.0 / np.sqrt(width)
    cosine = (np.cos(angle) * norm).astype(np.float32)
    sine = (np.sin(angle) * norm).astype(np.float32)

    def left(r, i):
        return np.concatenate(
            [np.concatenate([r, -i], 1), np.concatenate([i, r], 1)], 0
        ).astype(BF16)

    def right(r, i):
        return np.concatenate(
            [np.concatenate([r, i], 1), np.concatenate([-i, r], 1)], 0
        ).astype(BF16)

    h = width // 2
    split = []
    for parity in (0, 1):
        split.append(left(cosine[parity::2, :h], -sine[parity::2, :h]))
    for parity in (0, 1):
        split.append(left(cosine[:h, parity::2], sine[:h, parity::2]))
    columns = [right(cosine[:h, k::2], -sine[:h, k::2]) for k in (0, 1)]
    columns += [right(cosine[k::2, :h], sine[k::2, :h]) for k in (0, 1)]
    return np.stack(split), np.stack(columns)


def lane_index(shape):
    return lax.broadcasted_iota(jnp.int32, shape, len(shape) - 1)


def pack_high(re, im):
    return jnp.where(lane_index(re.shape) < HALF, pltpu.roll(re, HALF, re.ndim - 1), im)


def pack_low(re, im):
    return jnp.where(lane_index(re.shape) < HALF, re, pltpu.roll(im, HALF, im.ndim - 1))


def dot(a, b):
    return jnp.dot(a, b, preferred_element_type=F32)


def join(parts, axis):
    return jnp.concatenate(parts, axis)


def forward(xr, xi, left, right):
    h = xr.shape[0] // 2
    sums = join([xr[:h] + xr[h:], xi[:h] + xi[h:]], 0).astype(BF16)
    gaps = join([xr[:h] - xr[h:], xi[:h] - xi[h:]], 0).astype(BF16)
    even, odd = dot(left[0], sums), dot(left[1], gaps)

    def halves(y, sign):
        y = y[:, :h] + y[:, h:] if sign > 0 else y[:, :h] - y[:, h:]
        return join([y[:h], y[h:]], 1).astype(BF16)

    low = dot(join([halves(even, 1), halves(odd, 1)], 0), right[0])
    high = dot(join([halves(even, -1), halves(odd, -1)], 0), right[1])
    return join([low[:, :h], high[:, :h]], 1), join([low[:, h:], high[:, h:]], 1)


def inverse(xr, xi, left, right):
    h = xr.shape[0] // 2
    e = dot(left[2], join([xr[:h], xi[:h]], 0).astype(BF16))
    o = dot(left[3], join([xr[h:], xi[h:]], 0).astype(BF16))
    top, bottom = (e + o).astype(BF16), (e - o).astype(BF16)

    def columns(part):
        lanes = slice(part * h, part * h + h)
        return join(
            [join([y[:h, lanes], y[h:, lanes]], 1) for y in (top, bottom)], 0
        )

    a, b = dot(columns(0), right[2]), dot(columns(1), right[3])
    plus, minus = a + b, a - b
    return join([plus[:, :h], minus[:, :h]], 1), join([plus[:, h:], minus[:, h:]], 1)


def step_kernel(
    offsets, objects, probe_in, kernel_in, measured_in, left_in, right_in,
    out,
    ext1, ext2, probe, turned, plain, kern, measured, left, right, held, pieces1, pieces2,
    strips, edge1, edge2, g_rows1, g_rows2, g_cols1, g_cols2, r_rows1, r_rows2, r_cols1, r_cols2,
    load_sems, send, recv,
):
    tile = objects.shape[1]
    width = probe.shape[1]
    h = width // 2
    n_tiles = tile // LANES
    positions = measured.shape[0]
    extent = tile + 2 * HALO
    pitch = width + HALO
    pieces = (pieces1, pieces2)
    inner = pl.ds(HALO, tile)
    up_rows, down_rows = pl.ds(0, HALO), pl.ds(HALO + tile, HALO)
    first_rows, last_rows = pl.ds(HALO, HALO), pl.ds(tile, HALO)
    body_tiles = pl.ds(1, n_tiles)
    ext = (ext1, ext2)
    edge = (edge1, edge2)
    g_rows, g_cols = (g_rows1, g_rows2), (g_cols1, g_cols2)
    r_rows, r_cols = (r_rows1, r_rows2), (r_cols1, r_cols2)

    me_r, me_c = lax.axis_index("row"), lax.axis_index("col")
    n_r, n_c = lax.axis_size("row"), lax.axis_size("col")
    north, south = lax.rem(me_r + n_r - 1, n_r), lax.rem(me_r + 1, n_r)
    west, east = lax.rem(me_c + n_c - 1, n_c), lax.rem(me_c + 1, n_c)
    has_n, has_s, has_w, has_e = me_r > 0, me_r < n_r - 1, me_c > 0, me_c < n_c - 1
    others = [(north, me_c), (south, me_c), (me_r, west), (me_r, east),
              (north, west), (north, east), (south, west), (south, east)]
    here = [has_n, has_s, has_w, has_e, has_n & has_w, has_n & has_e, has_s & has_w, has_s & has_e]
    opposite = [1, 0, 3, 2, 7, 6, 5, 4]
    for ref in (r_rows1, r_rows2, r_cols1, r_cols2):
        ref[...] = jnp.zeros_like(ref)
    barrier = pltpu.get_barrier_semaphore()
    neighbours = 0
    for other, there in zip(others, here):
        neighbours = neighbours + there.astype(jnp.int32)

        @pl.when(there)
        def _():
            pl.semaphore_signal(barrier, inc=1, device_id=other, device_id_type=MESH)

    loads = []

    def load(src, dst):
        copy = pltpu.make_async_copy(src, dst, load_sems.at[len(loads)])
        copy.start()
        loads.append(copy)

    for s in range(2):
        for t in range(n_tiles):
            load(objects.at[pl.ds(2 * s, 2), :, pl.ds(t * LANES, LANES)], ext[s].at[:, 1 + t, inner, :])
    load(probe_in, probe)
    for t in range(width // LANES):
        load(kernel_in.at[:, :, pl.ds(t * LANES, LANES)], plain.at[:, t])
    load(left_in, left)
    load(right_in, right)
    for t in range(width // LANES):
        load(measured_in.at[0, 0, :, :, pl.ds(t * LANES, LANES)], measured.at[:, t])

    def exchange(phase, to_west, to_east, base, from_west, from_east, above, below, from_up, from_down, between):
        main = pl.ds(base, tile)
        upper = pl.ds(0, HALO)
        lower = pl.ds(base + tile + base - HALO, HALO)
        landed = inner
        moves = [
            (to_west.at[main], from_east.at[landed], 2),
            (to_east.at[main], from_west.at[landed], 3),
            (to_west.at[upper], from_east.at[down_rows], 4),
            (to_east.at[upper], from_west.at[down_rows], 5),
            (to_west.at[lower], from_east.at[up_rows], 6),
            (to_east.at[lower], from_west.at[up_rows], 7),
            (above, from_down, 0),
            (below, from_up, 1),
        ]
        copies = []
        for src, dst, k in moves:
            if k == 0:
                between()
            copy = pltpu.make_async_remote_copy(
                src_ref=src, dst_ref=dst, send_sem=send.at[phase, k], recv_sem=recv.at[phase, k],
                device_id=others[k], device_id_type=MESH,
            )
            pl.when(here[k])(copy.start)
            copies.append((copy, k))
        return copies

    def finish(copies):
        for copy, k in copies:
            pl.when(here[k])(copy.wait_send)
            pl.when(here[opposite[k]])(copy.wait_recv)

    def send_halo(s):
        e = ext[s]
        return exchange(
            s,
            strips.at[s, 0], strips.at[s, 1], 0, edge[s].at[0], edge[s].at[1],
            e.at[:, body_tiles, first_rows, :], e.at[:, body_tiles, last_rows, :],
            e.at[:, body_tiles, up_rows, :], e.at[:, body_tiles, down_rows, :],
            lambda: None,
        )

    def send_gradient(s):
        g, r = g_rows[s], r_rows[s]
        c, d = g_cols[s], r_cols[s]
        gather_sides(s)
        return exchange(
            2 + s, c.at[0], c.at[1], HALO, d.at[0], d.at[1],
            g.at[0], g.at[1], r.at[0], r.at[1], lambda: gather_ends(s),
        )

    for copy in loads[:n_tiles]:
        copy.wait()

    def pack(s):
        strips[s, 0] = pack_low(ext[s][0, 1, inner, :], ext[s][1, 1, inner, :])
        strips[s, 1] = pack_high(ext[s][0, n_tiles, inner, :], ext[s][1, n_tiles, inner, :])
    pack(0)

    def clear(i, carry):
        rows = pl.ds(pl.multiple_of(i * pitch, HALO), HALO)
        for ref in pieces:
            ref[:, :, rows, :] = jnp.zeros((2, 3, HALO, LANES), F32)
        return carry

    lax.fori_loop(0, positions + 1, clear, 0)
    pl.semaphore_wait(barrier, neighbours)
    halo1 = send_halo(0)

    for copy in loads[n_tiles:]:
        copy.wait()
    pack(1)
    source = lax.broadcasted_iota(jnp.int32, (width, width), 0)
    target = lane_index((width, width))
    order = (source == jnp.where(target < h, 2 * target, 2 * target - (width - 1))).astype(F32)

    def by_parity(whole):
        return jnp.dot(
            whole, order, precision=lax.Precision.HIGHEST, preferred_element_type=F32
        )

    for k in range(2):
        whole = by_parity(join([plain[k, 0], plain[k, 1]], 1))
        plain[k, 0] = whole[:, :h]
        plain[k, 1] = whole[:, h:]
    for k in range(2):
        for parity in range(2):
            for t in range(width // LANES):
                kern[k, pl.ds(parity * h, h), pl.ds(t * LANES, LANES)] = plain[
                    k, t, pl.ds(parity, h, stride=2), :
                ]

    def where_of(p):
        top = offsets[0, 0, 0, p] + HALO
        start = offsets[0, 0, 1, p] + LANES
        q = start // LANES
        return top, q, start - q * LANES

    def turn(p, carry):
        whole = by_parity(join([measured[p, 0], measured[p, 1]], 1))
        measured[p, 0] = whole[:, :h]
        measured[p, 1] = whole[:, h:]
        r = where_of(p)[2]
        for k in range(2):
            turned[p, k] = pltpu.roll(probe[k], r, 1)
        return carry

    lax.fori_loop(0, positions, turn, 0)
    halo2 = send_halo(1)

    def unpack_halo(s):
        both = edge[s][0]
        ext[s][0, 0] = pltpu.roll(both, HALF, 1)
        ext[s][1, 0] = both
        both = edge[s][1]
        ext[s][0, n_tiles + 1] = both
        ext[s][1, n_tiles + 1] = pltpu.roll(both, HALF, 1)

    def window(s, plane, p):
        top, q, r = where_of(p)
        rows = pl.ds(top, width)
        keep = lane_index((width, LANES)) >= r
        first = jnp.where(keep, ext[s][plane, q, rows, :], ext[s][plane, q + 2, rows, :])
        return jnp.concatenate([first, ext[s][plane, q + 1, rows, :]], 1)

    def put(s, p, c, value):
        rows = pl.ds(HALO + p * pitch, width)
        keep = lane_index((width, LANES)) >= where_of(p)[2]
        first = value[:, :LANES]
        pieces[s][c, 0, rows, :] = jnp.where(keep, first, 0.0)
        pieces[s][c, 1, rows, :] = value[:, LANES:]
        pieces[s][c, 2, rows, :] = jnp.where(keep, 0.0, first)

    finish(halo1)
    unpack_halo(0)

    def stage_a(p, carry):
        pr, pim = turned[p, 0], turned[p, 1]
        o1r, o1i = window(0, 0, p), window(0, 1, p)
        fr, fi = forward(pr * o1r - pim * o1i, pr * o1i + pim * o1r, left, right)
        kr, kim = kern[0], kern[1]
        sr, si = inverse(kr * fr - kim * fi, kr * fi + kim * fr, left, right)
        held[p, 0] = sr
        held[p, 1] = si
        return carry

    lax.fori_loop(0, positions, stage_a, 0, unroll=3)

    finish(halo2)
    unpack_halo(1)

    def stage_b(p, carry):
        sr, si = held[p, 0], held[p, 1]
        o2r, o2i = window(1, 0, p), window(1, 1, p)
        zr, zi = forward(sr * o2r - si * o2i, sr * o2i + si * o2r, left, right)
        amplitude = jnp.concatenate(
            [
                jnp.concatenate(
                    [measured[p, t, pl.ds(k, h, stride=2), :] for t in range(width // LANES)], 1
                )
                for k in range(2)
            ],
            0,
        )
        factor = 1.0 - amplitude * lax.rsqrt(zr * zr + zi * zi + 1.0)
        gr, gi = inverse(zr * factor, zi * factor, left, right)
        sr, si = held[p, 0], held[p, 1]
        put(1, p, 0, sr * gr + si * gi)
        put(1, p, 1, sr * gi - si * gr)
        held[p, 0] = gr
        held[p, 1] = gi
        return carry

    lax.fori_loop(0, positions, stage_b, 0, unroll=3)

    def gather(s, t, row):
        totals = [jnp.zeros((HALO, LANES), F32)] * 2
        for p in range(positions):
            top, q, _ = spots[p]
            ahead = row - top
            inside = (t >= q) & (t <= q + 2) & (ahead > -HALO) & (ahead < width)
            slot = jnp.where(inside, t - q, 0)
            rows = pl.ds(jnp.where(inside, HALO + p * pitch + ahead, 0), HALO)
            totals = [totals[c] + pieces[s][c, slot, rows, :] for c in range(2)]
        return totals

    def gather_sides(s):
        def sides(i, carry):
            row = pl.multiple_of(i * HALO, HALO)
            rows = pl.ds(row, HALO)
            g_cols[s][0, rows, :] = pack_high(*gather(s, 0, row))
            g_cols[s][1, rows, :] = pack_low(*gather(s, n_tiles + 1, row))
            return carry

        lax.fori_loop(0, extent // HALO, sides, 0)

    def gather_ends(s):
        def ends(i, carry):
            for k in range(2):
                totals = gather(s, 1 + i, k * (HALO + tile))
                for c in range(2):
                    g_rows[s][k, c, i] = totals[c]
            return carry

        lax.fori_loop(0, n_tiles, ends, 0)

    def gather_inner(s):
        def chunk(i, carry):
            row = pl.multiple_of(i * HALO, HALO)
            for t in range(n_tiles):
                totals = gather(s, t + 1, row + HALO)
                for c in range(2):
                    out[2 * s + c, pl.ds(row, HALO), pl.ds(t * LANES, LANES)] = (
                        ext[s][c, t + 1, pl.ds(row + HALO, HALO), :] - RATE * totals[c]
                    )
            return carry

        lax.fori_loop(0, tile // HALO, chunk, 0)

    def subtract(plane, rows, t, value):
        lanes = pl.ds(t * LANES, LANES)
        out[plane, rows, lanes] = out[plane, rows, lanes] - RATE * value

    def add_borders(s):
        begin, end = pl.ds(0, HALO), pl.ds(tile - HALO, HALO)
        for t in range(n_tiles):
            for c in range(2):
                subtract(2 * s + c, begin, t, r_rows[s][0, c, t])
                subtract(2 * s + c, end, t, r_rows[s][1, c, t])
        for rows, source in ((pl.ds(0, tile), inner), (begin, up_rows), (end, down_rows)):
            both = r_cols[s][0, source, :]
            low = lane_index(both.shape) < HALF
            subtract(2 * s, rows, 0, jnp.where(low, both, 0.0))
            subtract(2 * s + 1, rows, 0, jnp.where(low, pltpu.roll(both, HALF, 1), 0.0))
            both = r_cols[s][1, source, :]
            subtract(2 * s, rows, n_tiles - 1, jnp.where(low, 0.0, pltpu.roll(both, HALF, 1)))
            subtract(2 * s + 1, rows, n_tiles - 1, jnp.where(low, 0.0, both))

    spots = [where_of(p) for p in range(positions)]
    sent2 = send_gradient(1)

    def stage_c(p, carry):
        gr, gi = held[p, 0], held[p, 1]
        o2r, o2i = window(1, 0, p), window(1, 1, p)
        ur, ui = forward(o2r * gr + o2i * gi, o2r * gi - o2i * gr, left, right)
        kr, kim = kern[0], kern[1]
        wr, wi = inverse(kr * ur + kim * ui, kr * ui - kim * ur, left, right)
        pr, pim = turned[p, 0], turned[p, 1]
        put(0, p, 0, pr * wr + pim * wi)
        put(0, p, 1, pr * wi - pim * wr)
        return carry

    lax.fori_loop(0, positions, stage_c, 0, unroll=3)

    sent1 = send_gradient(0)
    gather_inner(1)
    gather_inner(0)
    finish(sent2)
    add_borders(1)
    finish(sent1)
    add_borders(0)


def per_device(objects, probe, kernel, measured, offsets):
    tile, width = objects.shape[1], probe.shape[1]
    n_tiles = tile // LANES
    extent = tile + 2 * HALO
    left, right = tables(width)
    positions = measured.shape[2]
    ext = pltpu.VMEM((2, n_tiles + 2, extent, LANES), F32)
    planes = pltpu.VMEM((positions, 2, width, width), F32)
    pieces = pltpu.VMEM((2, 3, positions * (width + HALO) + HALO, LANES), F32)
    cols = pltpu.VMEM((2, extent, LANES), F32)
    rows = pltpu.VMEM((2, 2, n_tiles, HALO, LANES), F32)
    dma = pltpu.SemaphoreType.DMA
    return pl.pallas_call(
        step_kernel,
        out_shape=pltpu.VMEM(objects.shape, F32),
        in_specs=[pl.BlockSpec(memory_space=pltpu.SMEM)] + [ANY] * 6,
        out_specs=pl.BlockSpec(memory_space=pltpu.VMEM),
        scratch_shapes=[
            ext,
            ext,
            pltpu.VMEM(probe.shape, F32),
            planes,
            pltpu.VMEM((2, width // LANES, width, LANES), F32),
            pltpu.VMEM(probe.shape, F32),
            pltpu.VMEM((positions, width // LANES, width, LANES), F32),
            pltpu.VMEM(left.shape, BF16),
            pltpu.VMEM(right.shape, BF16),
            planes,
            pieces,
            pieces,
            pltpu.VMEM((2, 2, tile, LANES), F32),
            cols, cols, rows, rows, cols, cols, rows, rows, cols, cols,
            dma((24,)), dma((4, 8)), dma((4, 8)),
        ],
        compiler_params=pltpu.CompilerParams(
            vmem_limit_bytes=58 * 2**20, collective_id=0, has_side_effects=True
        ),
        name="step",
    )(jnp.swapaxes(offsets, 2, 3), objects, probe, kernel, measured, jnp.asarray(left), jnp.asarray(right))


def solution(mesh):
    return jax.shard_map(
        per_device,
        mesh=mesh,
        in_specs=(
            P(None, "row", "col"),
            P(),
            P(),
            P("row", "col", None, None, None),
            P("row", "col", None, None),
        ),
        out_specs=P(None, "row", "col"),
        check_vma=False,
    )
```

```python
import functools

import jax
import jax.numpy as jnp
import numpy as np
from jax import lax
from jax.experimental import pallas as pl
from jax.experimental.pallas import tpu as pltpu
from jax.sharding import PartitionSpec as P

HALO = 64
RATE = 0.5
LANES = 128
HALF = 64
MESH = pl.DeviceIdType.MESH
BF16 = jnp.bfloat16
F32 = jnp.float32
ANY = pl.BlockSpec(memory_space=pl.ANY)


@functools.cache
def tables(width):
    index = np.arange(width)
    angle = 2.0 * np.pi / width * (index[:, None] * index[None, :] % width)
    norm = 1.0 / np.sqrt(width)
    cosine = (np.cos(angle) * norm).astype(np.float32)
    sine = (np.sin(angle) * norm).astype(np.float32)

    def left(r, i):
        return np.concatenate(
            [np.concatenate([r, -i], 1), np.concatenate([i, r], 1)], 0
        ).astype(BF16)

    def right(r, i):
        return np.concatenate(
            [np.concatenate([r, i], 1), np.concatenate([-i, r], 1)], 0
        ).astype(BF16)

    h = width // 2
    split = []
    for parity in (0, 1):
        split.append(left(cosine[parity::2, :h], -sine[parity::2, :h]))
    for parity in (0, 1):
        split.append(left(cosine[:h, parity::2], sine[:h, parity::2]))
    columns = [right(cosine[:h, k::2], -sine[:h, k::2]) for k in (0, 1)]
    columns += [right(cosine[k::2, :h], sine[k::2, :h]) for k in (0, 1)]
    return np.stack(split), np.stack(columns)


def lane_index(shape):
    return lax.broadcasted_iota(jnp.int32, shape, len(shape) - 1)


def pack_high(re, im):
    return jnp.where(lane_index(re.shape) < HALF, pltpu.roll(re, HALF, re.ndim - 1), im)


def pack_low(re, im):
    return jnp.where(lane_index(re.shape) < HALF, re, pltpu.roll(im, HALF, im.ndim - 1))


def dot(a, b):
    return jnp.dot(a, b, preferred_element_type=F32)


def join(parts, axis):
    return jnp.concatenate(parts, axis)


def forward(xr, xi, left, right):
    h = xr.shape[0] // 2
    sums = join([xr[:h] + xr[h:], xi[:h] + xi[h:]], 0).astype(BF16)
    gaps = join([xr[:h] - xr[h:], xi[:h] - xi[h:]], 0).astype(BF16)
    even, odd = dot(left[0], sums), dot(left[1], gaps)

    def halves(y, sign):
        y = y[:, :h] + y[:, h:] if sign > 0 else y[:, :h] - y[:, h:]
        return join([y[:h], y[h:]], 1).astype(BF16)

    low = dot(join([halves(even, 1), halves(odd, 1)], 0), right[0])
    high = dot(join([halves(even, -1), halves(odd, -1)], 0), right[1])
    return join([low[:, :h], high[:, :h]], 1), join([low[:, h:], high[:, h:]], 1)


def inverse(xr, xi, left, right):
    h = xr.shape[0] // 2
    e = dot(left[2], join([xr[:h], xi[:h]], 0).astype(BF16))
    o = dot(left[3], join([xr[h:], xi[h:]], 0).astype(BF16))
    top, bottom = (e + o).astype(BF16), (e - o).astype(BF16)

    def columns(part):
        lanes = slice(part * h, part * h + h)
        return join(
            [join([y[:h, lanes], y[h:, lanes]], 1) for y in (top, bottom)], 0
        )

    a, b = dot(columns(0), right[2]), dot(columns(1), right[3])
    plus, minus = a + b, a - b
    return join([plus[:, :h], minus[:, :h]], 1), join([plus[:, h:], minus[:, h:]], 1)


def step_kernel(
    offsets, objects, probe_in, kernel_in, measured_in, left_in, right_in,
    out,
    ext1, ext2, probe, turned, plain, kern, measured, left, right, held, pieces1, pieces2,
    strips, edge1, edge2, g_rows1, g_rows2, g_cols1, g_cols2, r_rows1, r_rows2, r_cols1, r_cols2,
    load_sems, send, recv,
):
    tile = objects.shape[1]
    width = probe.shape[1]
    h = width // 2
    n_tiles = tile // LANES
    positions = measured.shape[0]
    extent = tile + 2 * HALO
    pitch = width + HALO
    pieces = (pieces1, pieces2)
    inner = pl.ds(HALO, tile)
    up_rows, down_rows = pl.ds(0, HALO), pl.ds(HALO + tile, HALO)
    first_rows, last_rows = pl.ds(HALO, HALO), pl.ds(tile, HALO)
    body_tiles = pl.ds(1, n_tiles)
    ext = (ext1, ext2)
    edge = (edge1, edge2)
    g_rows, g_cols = (g_rows1, g_rows2), (g_cols1, g_cols2)
    r_rows, r_cols = (r_rows1, r_rows2), (r_cols1, r_cols2)

    me_r, me_c = lax.axis_index("row"), lax.axis_index("col")
    n_r, n_c = lax.axis_size("row"), lax.axis_size("col")
    north, south = lax.rem(me_r + n_r - 1, n_r), lax.rem(me_r + 1, n_r)
    west, east = lax.rem(me_c + n_c - 1, n_c), lax.rem(me_c + 1, n_c)
    has_n, has_s, has_w, has_e = me_r > 0, me_r < n_r - 1, me_c > 0, me_c < n_c - 1
    others = [(north, me_c), (south, me_c), (me_r, west), (me_r, east),
              (north, west), (north, east), (south, west), (south, east)]
    here = [has_n, has_s, has_w, has_e, has_n & has_w, has_n & has_e, has_s & has_w, has_s & has_e]
    opposite = [1, 0, 3, 2, 7, 6, 5, 4]
    loads = []

    def load(src, dst):
        copy = pltpu.make_async_copy(src, dst, load_sems.at[len(loads)])
        copy.start()
        loads.append(copy)

    for s in range(2):
        for t in range(n_tiles):
            load(objects.at[pl.ds(2 * s, 2), :, pl.ds(t * LANES, LANES)], ext[s].at[:, 1 + t, inner, :])
    load(probe_in, probe)
    for t in range(width // LANES):
        load(kernel_in.at[:, :, pl.ds(t * LANES, LANES)], plain.at[:, t])
    load(left_in, left)
    load(right_in, right)
    for t in range(width // LANES):
        load(measured_in.at[0, 0, :, :, pl.ds(t * LANES, LANES)], measured.at[:, t])

    for ref in (r_rows1, r_rows2, r_cols1, r_cols2):
        ref[...] = jnp.zeros_like(ref)
    barrier = pltpu.get_barrier_semaphore()
    neighbours = 0
    for other, there in zip(others, here):
        neighbours = neighbours + there.astype(jnp.int32)

        @pl.when(there)
        def _():
            pl.semaphore_signal(barrier, inc=1, device_id=other, device_id_type=MESH)

    def exchange(phase, to_west, to_east, base, from_west, from_east, above, below, from_up, from_down, between):
        main = pl.ds(base, tile)
        upper = pl.ds(0, HALO)
        lower = pl.ds(base + tile + base - HALO, HALO)
        landed = inner
        moves = [
            (to_west.at[main], from_east.at[landed], 2),
            (to_east.at[main], from_west.at[landed], 3),
            (to_west.at[upper], from_east.at[down_rows], 4),
            (to_east.at[upper], from_west.at[down_rows], 5),
            (to_west.at[lower], from_east.at[up_rows], 6),
            (to_east.at[lower], from_west.at[up_rows], 7),
            (above, from_down, 0),
            (below, from_up, 1),
        ]
        copies = []
        for src, dst, k in moves:
            if k == 0:
                between()
            copy = pltpu.make_async_remote_copy(
                src_ref=src, dst_ref=dst, send_sem=send.at[phase, k], recv_sem=recv.at[phase, k],
                device_id=others[k], device_id_type=MESH,
            )
            pl.when(here[k])(copy.start)
            copies.append((copy, k))
        return copies

    def finish(copies):
        for copy, k in copies:
            pl.when(here[k])(copy.wait_send)
            pl.when(here[opposite[k]])(copy.wait_recv)

    def send_halo(s, between):
        e = ext[s]
        return exchange(
            s,
            strips.at[s, 0], strips.at[s, 1], 0, edge[s].at[0], edge[s].at[1],
            e.at[:, body_tiles, first_rows, :], e.at[:, body_tiles, last_rows, :],
            e.at[:, body_tiles, up_rows, :], e.at[:, body_tiles, down_rows, :],
            between,
        )

    def send_gradient(s):
        g, r = g_rows[s], r_rows[s]
        c, d = g_cols[s], r_cols[s]
        gather_sides(s)
        return exchange(
            2 + s, c.at[0], c.at[1], HALO, d.at[0], d.at[1],
            g.at[0], g.at[1], r.at[0], r.at[1], lambda: gather_ends(s),
        )

    for copy in loads[:n_tiles]:
        copy.wait()

    def pack(s):
        strips[s, 0] = pack_low(ext[s][0, 1, inner, :], ext[s][1, 1, inner, :])
        strips[s, 1] = pack_high(ext[s][0, n_tiles, inner, :], ext[s][1, n_tiles, inner, :])
    pack(0)

    def clear(i, carry):
        rows = pl.ds(pl.multiple_of(i * pitch, HALO), HALO)
        for ref in pieces:
            ref[:, :, rows, :] = jnp.zeros((2, 3, HALO, LANES), F32)
        return carry

    lax.fori_loop(0, positions + 1, clear, 0)
    pl.semaphore_wait(barrier, neighbours)
    halo1 = send_halo(0, lambda: None)

    for copy in loads[n_tiles:]:
        copy.wait()
    pack(1)
    source = lax.broadcasted_iota(jnp.int32, (width, width), 0)
    target = lane_index((width, width))
    order = (source == jnp.where(target < h, 2 * target, 2 * target - (width - 1))).astype(F32)

    def by_parity(whole):
        return jnp.dot(
            whole, order, precision=lax.Precision.HIGHEST, preferred_element_type=F32
        )

    for k in range(2):
        whole = by_parity(join([plain[k, 0], plain[k, 1]], 1))
        plain[k, 0] = whole[:, :h]
        plain[k, 1] = whole[:, h:]
    for k in range(2):
        for parity in range(2):
            for t in range(width // LANES):
                kern[k, pl.ds(parity * h, h), pl.ds(t * LANES, LANES)] = plain[
                    k, t, pl.ds(parity, h, stride=2), :
                ]

    def where_of(p):
        top = offsets[0, 0, 0, p] + HALO
        start = offsets[0, 0, 1, p] + LANES
        q = start // LANES
        return top, q, start - q * LANES

    def turn(p, carry):
        whole = by_parity(join([measured[p, 0], measured[p, 1]], 1))
        measured[p, 0] = whole[:, :h]
        measured[p, 1] = whole[:, h:]
        r = where_of(p)[2]
        for k in range(2):
            turned[p, k] = pltpu.roll(probe[k], r, 1)
        return carry

    lax.fori_loop(0, positions, turn, 0)
    def unpack_halo(s):
        both = edge[s][0]
        ext[s][0, 0] = pltpu.roll(both, HALF, 1)
        ext[s][1, 0] = both
        both = edge[s][1]
        ext[s][0, n_tiles + 1] = both
        ext[s][1, n_tiles + 1] = pltpu.roll(both, HALF, 1)

    def window(s, plane, p):
        top, q, r = where_of(p)
        rows = pl.ds(top, width)
        keep = lane_index((width, LANES)) >= r
        first = jnp.where(keep, ext[s][plane, q, rows, :], ext[s][plane, q + 2, rows, :])
        return jnp.concatenate([first, ext[s][plane, q + 1, rows, :]], 1)

    def put(s, p, c, value):
        rows = pl.ds(HALO + p * pitch, width)
        keep = lane_index((width, LANES)) >= where_of(p)[2]
        first = value[:, :LANES]
        pieces[s][c, 0, rows, :] = jnp.where(keep, first, 0.0)
        pieces[s][c, 1, rows, :] = value[:, LANES:]
        pieces[s][c, 2, rows, :] = jnp.where(keep, 0.0, first)

    halo2 = send_halo(1, lambda: finish(halo1))
    unpack_halo(0)

    def stage_a(p, carry):
        pr, pim = turned[p, 0], turned[p, 1]
        o1r, o1i = window(0, 0, p), window(0, 1, p)
        fr, fi = forward(pr * o1r - pim * o1i, pr * o1i + pim * o1r, left, right)
        kr, kim = kern[0], kern[1]
        sr, si = inverse(kr * fr - kim * fi, kr * fi + kim * fr, left, right)
        held[p, 0] = sr
        held[p, 1] = si
        return carry

    lax.fori_loop(0, positions, stage_a, 0, unroll=3)

    finish(halo2)
    unpack_halo(1)

    def stage_b(p, carry):
        sr, si = held[p, 0], held[p, 1]
        o2r, o2i = window(1, 0, p), window(1, 1, p)
        zr, zi = forward(sr * o2r - si * o2i, sr * o2i + si * o2r, left, right)
        amplitude = jnp.concatenate(
            [
                jnp.concatenate(
                    [measured[p, t, pl.ds(k, h, stride=2), :] for t in range(width // LANES)], 1
                )
                for k in range(2)
            ],
            0,
        )
        factor = 1.0 - amplitude * lax.rsqrt(zr * zr + zi * zi + 1.0)
        gr, gi = inverse(zr * factor, zi * factor, left, right)
        sr, si = held[p, 0], held[p, 1]
        put(1, p, 0, sr * gr + si * gi)
        put(1, p, 1, sr * gi - si * gr)
        held[p, 0] = gr
        held[p, 1] = gi
        return carry

    lax.fori_loop(0, positions, stage_b, 0, unroll=3)

    far = 8 * extent

    def places(t):
        found = []
        for top, q, _ in spots:
            ahead = t - q
            near = (ahead >= 0) & (ahead <= 2)
            found.append((jnp.where(near, top, far), jnp.where(near, ahead, 0)))
        return found

    def gather(s, found, row):
        totals = [jnp.zeros((HALO, LANES), F32)] * 2
        for p, (top, slot) in enumerate(found):
            ahead = row - top
            inside = (ahead > -HALO) & (ahead < width)
            rows = pl.ds(jnp.where(inside, ahead + (HALO + p * pitch), 0), HALO)
            totals = [totals[c] + pieces[s][c, slot, rows, :] for c in range(2)]
        return totals

    def gather_sides(s):
        first, last = places(0), places(n_tiles + 1)

        def sides(i, carry):
            row = pl.multiple_of(i * HALO, HALO)
            rows = pl.ds(row, HALO)
            g_cols[s][0, rows, :] = pack_high(*gather(s, first, row))
            g_cols[s][1, rows, :] = pack_low(*gather(s, last, row))
            return carry

        lax.fori_loop(0, extent // HALO, sides, 0)

    def gather_ends(s):
        def ends(i, carry):
            found = places(1 + i)
            for k in range(2):
                totals = gather(s, found, k * (HALO + tile))
                for c in range(2):
                    g_rows[s][k, c, i] = totals[c]
            return carry

        lax.fori_loop(0, n_tiles, ends, 0)

    def gather_inner(s):
        def chunk(i, carry):
            row = pl.multiple_of(i * HALO, HALO)
            for t in range(n_tiles):
                totals = gather(s, places(t + 1), row + HALO)
                for c in range(2):
                    out[2 * s + c, pl.ds(row, HALO), pl.ds(t * LANES, LANES)] = (
                        ext[s][c, t + 1, pl.ds(row + HALO, HALO), :] - RATE * totals[c]
                    )
            return carry

        lax.fori_loop(0, tile // HALO, chunk, 0)

    def subtract(plane, rows, t, value):
        lanes = pl.ds(t * LANES, LANES)
        out[plane, rows, lanes] = out[plane, rows, lanes] - RATE * value

    def add_borders(s):
        begin, end = pl.ds(0, HALO), pl.ds(tile - HALO, HALO)
        for t in range(n_tiles):
            for c in range(2):
                subtract(2 * s + c, begin, t, r_rows[s][0, c, t])
                subtract(2 * s + c, end, t, r_rows[s][1, c, t])
        for rows, source in ((pl.ds(0, tile), inner), (begin, up_rows), (end, down_rows)):
            both = r_cols[s][0, source, :]
            low = lane_index(both.shape) < HALF
            subtract(2 * s, rows, 0, jnp.where(low, both, 0.0))
            subtract(2 * s + 1, rows, 0, jnp.where(low, pltpu.roll(both, HALF, 1), 0.0))
            both = r_cols[s][1, source, :]
            subtract(2 * s, rows, n_tiles - 1, jnp.where(low, 0.0, pltpu.roll(both, HALF, 1)))
            subtract(2 * s + 1, rows, n_tiles - 1, jnp.where(low, 0.0, both))

    spots = [where_of(p) for p in range(positions)]
    sent2 = send_gradient(1)

    def stage_c(p, carry):
        gr, gi = held[p, 0], held[p, 1]
        o2r, o2i = window(1, 0, p), window(1, 1, p)
        ur, ui = forward(o2r * gr + o2i * gi, o2r * gi - o2i * gr, left, right)
        kr, kim = kern[0], kern[1]
        wr, wi = inverse(kr * ur + kim * ui, kr * ui - kim * ur, left, right)
        pr, pim = turned[p, 0], turned[p, 1]
        put(0, p, 0, pr * wr + pim * wi)
        put(0, p, 1, pr * wi - pim * wr)
        return carry

    lax.fori_loop(0, positions, stage_c, 0, unroll=3)

    sent1 = send_gradient(0)
    gather_inner(1)
    gather_inner(0)
    finish(sent2)
    add_borders(1)
    finish(sent1)
    add_borders(0)


def per_device(objects, probe, kernel, measured, offsets):
    tile, width = objects.shape[1], probe.shape[1]
    n_tiles = tile // LANES
    extent = tile + 2 * HALO
    left, right = tables(width)
    positions = measured.shape[2]
    ext = pltpu.VMEM((2, n_tiles + 2, extent, LANES), F32)
    planes = pltpu.VMEM((positions, 2, width, width), F32)
    pieces = pltpu.VMEM((2, 3, positions * (width + HALO) + HALO, LANES), F32)
    cols = pltpu.VMEM((2, extent, LANES), F32)
    rows = pltpu.VMEM((2, 2, n_tiles, HALO, LANES), F32)
    dma = pltpu.SemaphoreType.DMA
    return pl.pallas_call(
        step_kernel,
        out_shape=pltpu.VMEM(objects.shape, F32),
        in_specs=[pl.BlockSpec(memory_space=pltpu.SMEM)] + [ANY] * 6,
        out_specs=pl.BlockSpec(memory_space=pltpu.VMEM),
        scratch_shapes=[
            ext,
            ext,
            pltpu.VMEM(probe.shape, F32),
            planes,
            pltpu.VMEM((2, width // LANES, width, LANES), F32),
            pltpu.VMEM(probe.shape, F32),
            pltpu.VMEM((positions, width // LANES, width, LANES), F32),
            pltpu.VMEM(left.shape, BF16),
            pltpu.VMEM(right.shape, BF16),
            planes,
            pieces,
            pieces,
            pltpu.VMEM((2, 2, tile, LANES), F32),
            cols, cols, rows, rows, cols, cols, rows, rows, cols, cols,
            dma((24,)), dma((4, 8)), dma((4, 8)),
        ],
        compiler_params=pltpu.CompilerParams(
            vmem_limit_bytes=58 * 2**20, collective_id=0, has_side_effects=True
        ),
        name="step",
    )(jnp.swapaxes(offsets, 2, 3), objects, probe, kernel, measured, jnp.asarray(left), jnp.asarray(right))


def solution(mesh):
    return jax.shard_map(
        per_device,
        mesh=mesh,
        in_specs=(
            P(None, "row", "col"),
            P(),
            P(),
            P("row", "col", None, None, None),
            P("row", "col", None, None),
        ),
        out_specs=P(None, "row", "col"),
        check_vma=False,
    )
```
